256 devices in a mesh: dp: 32 (over z_hi, y, core), level: 8 (over x, z_lo).
Axes of the slice: x: 4, y: 4, z: 8 (z_hi: 4, z_lo: 2; z = z_hi * 2 + z_lo), core: 2. Of those that a mesh axis runs over, the one named last changes fastest.
Arguments:
- token_ids: int32 [32, 8, 1536], P('dp', 'level'), may hold values from 0 to 1023
- decoded_mask: int32 [32, 8, 1536], P('dp', 'level'), may hold values 0 or 1
- levels_done: int32 [32], P('dp'), may hold values from 0 to 7
- code_tables: bfloat16 [8, 1024, 1024], P('level'), may hold values from -6 to 6
- mask_vectors: bfloat16 [8, 1024], P('level'), may hold values from -6 to 6
- w_qkv: bfloat16 [3, 1024, 1024], P(None, 'dp', 'level'), may hold values from -6 to 6
- w_out: bfloat16 [1024, 1024], P('level', 'dp'), may hold values from -0.1875 to 0.1875
- w_expand: bfloat16 [1024, 2048], P('dp'), may hold values from -0.1875 to 0.1875
- w_depth: bfloat16 [5, 1024], replicated, may hold values from -2.5 to 2.5
- w_project: bfloat16 [1024, 1024], P('dp'), may hold values from -0.1875 to 0.1875
- level_heads: bfloat16 [8, 1024, 1024], P('level'), may hold values from -0.1875 to 0.1875
Outputs:
- logits: bfloat16 [32, 8, 1536, 1024], P('dp', 'level')
The draws below stay inside these ranges and needn't reach their ends.
Inputs may be any that keep to these rules, and one draw needn't show every extreme that they name: `levels_done`: levels below it are fully decoded; the level equal to it is the one being decoded.
All inputs are finite; a program needn't handle non-finite values. No bound on the sum of `decoded_mask` on one device may be relied on, other than what follows from the above.
Results may differ from the reference program's by a relative error of at most 0.006.
Values may be sent and summed in bfloat16 or wider, within the bound.
A program may use at most 128 MiB of HBM per device.

```python
import jax
import jax.numpy as jnp
from jax import lax

D = 1024
HEADS = 16
VOCAB = 1024
FRAMES = 1536
KERNEL = 5
HEAD_DIM = 64
LEVELS = 8
CLIPS = 32


def draw_w_qkv(key, part):
    spread = D ** (-0.5)
    weights = jax.random.normal(jax.random.fold_in(key, 11), (3, D, D), jnp.float32) * spread
    weights = jnp.clip(weights, -6.0 * spread, 6.0 * spread)
    return jnp.clip(weights, -6.0, 6.0).astype(jnp.bfloat16)


def with_ends(values, key, low, top_value):
    longest = values.shape.index(max(values.shape))
    spots = []
    for shift in (0, 1):
        where = [jax.random.randint(jax.random.fold_in(key, axis), (), 0, length) for axis, length in enumerate(values.shape)]
        where[longest] = (where[longest] + shift) % values.shape[longest]
        spots.append(tuple(where))
    return values.at[spots[0]].set(low).at[spots[1]].set(top_value)


def block_scale(own_key, shape, split, low, top_value):
    gain = 1.0
    for dim, shards_of in split:
        steps = jax.random.uniform(jax.random.fold_in(jax.random.fold_in(own_key, 6), dim), (shards_of,), jnp.float32, low / len(split), top_value / len(split))
        gain = gain * jnp.repeat(jnp.exp(steps), shape[dim] // shards_of).reshape((-1,) + (1,) * (len(shape) - 1 - dim))
    return gain


def centred(stream_key, extent, width, bound, pieces=(), held_as=jnp.bfloat16):
    array = jax.random.normal(stream_key, extent, jnp.float32) * width
    if len(pieces) > 0:
        array = block_scale(stream_key, extent, pieces, -0.22, 0.18) * array
    return jnp.clip(array, min=-bound, max=bound).astype(held_as)


def setup_inputs(seed: int = 0) -> dict:
    streams_of = jax.random.split(jax.random.key(seed), 12)
    return {
        "token_ids": with_ends(jax.random.randint(streams_of[0], (CLIPS, LEVELS, FRAMES), 0, VOCAB), jax.random.fold_in(streams_of[0], 1), 0, VOCAB - 1).astype(jnp.int32),
        "decoded_mask": with_ends((jax.random.randint(streams_of[1], (CLIPS, LEVELS, FRAMES), 0, 2) < 1).astype(jnp.int32), jax.random.fold_in(streams_of[1], 1), 0, 1),
        "levels_done": with_ends(jax.random.randint(streams_of[2], (CLIPS,), 0, LEVELS), jax.random.fold_in(streams_of[2], 1), 0, LEVELS - 1).astype(jnp.int32),
        "code_tables": centred(streams_of[3], (LEVELS, VOCAB, D), 1.0, 6.0, ((0, 8),)),
        "mask_vectors": centred(streams_of[4], (LEVELS, D), 1.0, 6.0, ((0, 8),)),
        "w_qkv": draw_w_qkv(jax.random.fold_in(streams_of[11], 71), 0),
        "w_out": centred(streams_of[6], (D, D), D ** -0.5, 0.1875, ((0, 8), (1, 32))),
        "w_expand": centred(streams_of[7], (D, 2 * D), D ** -0.5, 0.1875, ((0, 32),)),
        "w_depth": centred(streams_of[8], (KERNEL, D), KERNEL ** -0.5, 2.5),
        "w_project": centred(streams_of[9], (D, D), D ** -0.5, 0.1875, ((0, 32),)),
        "level_heads": centred(streams_of[10], (LEVELS, D, VOCAB), D ** -0.5, 0.1875, ((0, 8),)),
    }


def layer_norm(values):
    centered = values - lax.optimization_barrier(jnp.mean(values, axis=-1, keepdims=True))
    variance = lax.optimization_barrier(jnp.mean(centered * centered, axis=-1, keepdims=True))
    return centered * lax.rsqrt(variance + 1e-05)

def clip_step(token_ids, decoded_mask, levels_done, code_tables, mask_vectors, w_qkv, w_out, w_expand, w_depth, w_project, level_heads):
    level_ids = jnp.arange(LEVELS, dtype=jnp.int32)[:, None]
    use_token = (level_ids < levels_done) | (level_ids == levels_done) & (decoded_mask == 1)
    picked = jax.vmap(lambda table_one, ids_one: jnp.take(table_one, ids_one, axis=0))(code_tables, token_ids.astype(jnp.int32)).astype(jnp.float32)
    terms = jnp.where(use_token[:, :, None], picked, mask_vectors.astype(jnp.float32)[:, None, :])
    embedded = lax.optimization_barrier(jnp.sum(terms, axis=0))
    normed = layer_norm(embedded).astype(jnp.bfloat16)
    queries = jnp.dot(normed, w_qkv[0], preferred_element_type=jnp.float32).astype(jnp.bfloat16)
    key_rows = jnp.dot(normed, w_qkv[1], preferred_element_type=jnp.float32).astype(jnp.bfloat16)
    value_rows = jnp.dot(normed, w_qkv[2], preferred_element_type=jnp.float32).astype(jnp.bfloat16)
    queries, key_rows, value_rows = lax.optimization_barrier((queries, key_rows, value_rows))
    query_three = queries.astype(jnp.float32).reshape(FRAMES, HEADS, HEAD_DIM)
    key_three = key_rows.astype(jnp.float32).reshape(FRAMES, HEADS, HEAD_DIM)
    value_three = value_rows.astype(jnp.float32).reshape(FRAMES, HEADS, HEAD_DIM)
    scores = jnp.einsum('qhd,khd->hqk', query_three, key_three) * HEAD_DIM ** (-0.5)
    row_max = lax.optimization_barrier(jnp.max(scores, axis=-1, keepdims=True))
    weights = jnp.exp(scores - row_max)
    weight_sum = lax.optimization_barrier(jnp.sum(weights, axis=-1))
    rounded = lax.optimization_barrier(weights.astype(jnp.bfloat16)).astype(jnp.float32)
    mixture = jnp.einsum('hqk,khd->qhd', rounded, value_three) / weight_sum.T[:, :, None]
    attended = mixture.reshape(FRAMES, D).astype(jnp.bfloat16)
    after_attn = embedded + jnp.dot(attended, w_out, preferred_element_type=jnp.float32)
    normed_two = layer_norm(after_attn).astype(jnp.bfloat16)
    gate_linear = jnp.dot(normed_two, w_expand, preferred_element_type=jnp.float32)
    gated = (gate_linear[:, :D] * jax.nn.sigmoid(gate_linear[:, D:])).astype(jnp.bfloat16)
    gated = lax.optimization_barrier(gated)
    half_width = KERNEL // 2
    padded = jnp.pad(gated.astype(jnp.float32), ((half_width, half_width), (0, 0)))
    conv = jnp.zeros((FRAMES, D), jnp.float32)
    for tap_index in range(KERNEL):
        conv = conv + padded[tap_index:tap_index + FRAMES] * w_depth[tap_index].astype(jnp.float32)
    activated = (conv * jax.nn.sigmoid(conv)).astype(jnp.bfloat16)
    after_conv = after_attn + jnp.dot(activated, w_project, preferred_element_type=jnp.float32)
    final_norm = layer_norm(after_conv).astype(jnp.bfloat16)
    return jax.vmap(lambda head_one: jnp.dot(final_norm, head_one, preferred_element_type=jnp.float32))(level_heads).astype(jnp.bfloat16)

def reference(token_ids, decoded_mask, levels_done, code_tables, mask_vectors, w_qkv, w_out, w_expand, w_depth, w_project, level_heads):

    def one_clip(clip_parts):
        return clip_step(clip_parts[0], clip_parts[1], clip_parts[2], code_tables, mask_vectors, w_qkv, w_out, w_expand, w_depth, w_project, level_heads)
    return lax.map(one_clip, (token_ids, decoded_mask, levels_done))
```

```python
import jax
import jax.numpy as jnp
from jax import lax
from jax.experimental import pallas as pl
from jax.experimental.pallas import tpu as pltpu
from jax.sharding import PartitionSpec as P

MESH = pl.DeviceIdType.MESH
BF16, F32 = jnp.bfloat16, jnp.float32

HEADS = 16
NZ, NY, NC = 4, 4, 2
NX, NL = 4, 2
LANES = 128
COPIES = 128


def layer_norm(values):
    centered = values - jnp.mean(values, axis=-1, keepdims=True)
    variance = jnp.mean(centered * centered, axis=-1, keepdims=True)
    return centered * lax.rsqrt(variance + 1e-05)


def step_kernel(
    sel_ref,
    fill_ref,
    taps_ref,
    table_hbm,
    wqkv_hbm,
    wout_hbm,
    wexp_hbm,
    wproj_hbm,
    head_hbm,
    out_hbm,
    table,
    head,
    weights,
    terms,
    partial,
    zsend,
    zrecv,
    own,
    normed,
    qkv_s,
    qkv_r,
    att_s,
    att_r,
    after,
    gated,
    halo,
    padded,
    active,
    final,
    staged,
    load_sem,
    store_sem,
    send_sem,
    recv_sem,
):
    groups = NX * NL
    rows, width = own.shape
    frames = rows * groups
    half = width // 2
    shard = weights.shape[3]

    dp = lax.axis_index("dp")
    lv = lax.axis_index("level")
    core = lax.rem(dp, NC)
    yy = lax.rem(dp // NC, NY)
    zh = dp // (NC * NY)
    xx, zl = lv // NL, lax.rem(lv, NL)
    zy = zh * NY + yy

    def level_of(dx, dz):
        return lax.rem(xx + dx + NX, NX) * NL + lax.rem(zl + dz, NL)

    def dp_of(dz, dy, dc):
        return (lax.rem(zh + dz + NZ, NZ) * NY + lax.rem(yy + dy + NY, NY)) * NC + lax.rem(core + dc, NC)

    x_up, x_down, z_mate = {"level": level_of(1, 0)}, {"level": level_of(-1, 0)}, {"level": level_of(0, 1)}
    z_up, z_down = {"dp": dp_of(1, 0, 0)}, {"dp": dp_of(-1, 0, 0)}
    y_up, y_down = {"dp": dp_of(0, 1, 0)}, {"dp": dp_of(0, -1, 0)}
    core_mate = {"dp": dp_of(0, 0, 1)}

    lane_at = pl.ds(pl.multiple_of(lv * LANES, LANES), LANES)
    loads = [
        pltpu.make_async_copy(table_hbm, table, load_sem.at[0]),
        pltpu.make_async_copy(wqkv_hbm, weights.at[zy, core, pl.ds(0, 3), :, lane_at], load_sem.at[1]),
        pltpu.make_async_copy(wout_hbm, weights.at[zy, core, 3, :, lane_at], load_sem.at[2]),
        pltpu.make_async_copy(wexp_hbm.at[:, pl.ds(0, width)], weights.at[zy, core, 4], load_sem.at[3]),
        pltpu.make_async_copy(wexp_hbm.at[:, pl.ds(width, width)], weights.at[zy, core, 5], load_sem.at[4]),
        pltpu.make_async_copy(wproj_hbm, weights.at[zy, core, 6], load_sem.at[5]),
        pltpu.make_async_copy(head_hbm, head, load_sem.at[6]),
    ]
    for load in loads:
        load.start()

    barrier = pltpu.get_barrier_semaphore()
    for k in range(1, groups):
        pl.semaphore_signal(barrier, inc=1, device_id={"level": level_of(k // NL, k % NL)}, device_id_type=MESH)
    for peer in (z_up, z_down, y_up, y_down, core_mate):
        pl.semaphore_signal(barrier, inc=1, device_id=peer, device_id_type=MESH)
    pl.semaphore_wait(barrier, groups + 4)

    used = [0]
    sent = []

    def make(src, dst, device, index):
        return pltpu.make_async_remote_copy(
            src_ref=src,
            dst_ref=dst,
            send_sem=send_sem.at[index],
            recv_sem=recv_sem.at[index],
            device_id=device,
            device_id_type=MESH,
        )

    def send(src, dst, device):
        copy = make(src, dst, device, used[0])
        used[0] += 1
        copy.start()
        sent.append(copy)
        return copy

    for load in loads[1:3]:
        load.wait()
    first = weights.at[zy, core, pl.ds(0, 4), :, lane_at]
    columns = [send(first, first, {"level": level_of(k // NL, k % NL)}) for k in range(1, groups)]

    codes = lax.broadcasted_iota(jnp.int32, (rows, table.shape[0]), 1).astype(F32)
    slots = lax.broadcasted_iota(jnp.int32, (rows, groups), 1)

    def term(dx, dz):
        dest = level_of(dx, dz)
        ids = jnp.sum(jnp.where(slots == dest, sel_ref[...], 0.0), axis=1, keepdims=True)
        onehot = jnp.where(ids == codes, 1.0, 0.0).astype(BF16)
        picked = jnp.dot(onehot, table[...], preferred_element_type=F32)
        terms[dest] = jnp.where(ids < 0.0, fill_ref[...].astype(F32), picked).astype(BF16)

    def col(d):
        return pl.ds(d * half, half)

    def ring_send(step, d, q):
        dx = -step if d == 0 else step
        block = terms.at[level_of(dx + NX, 1 - q), :, col(d)]
        return send(block, partial.at[d, step - 1, q], x_up if d == 0 else x_down)

    loads[0].wait()
    ring = {}
    for q in range(2):

        @pl.loop(0, 2)
        def _(i):
            term(2 * i + NX - 1, 1 - q)

        for d in range(2):
            ring[1, d, q] = ring_send(1, d, q)

    @pl.loop(0, 4)
    def _(i):
        term(2 + 2 * (i // 2), lax.rem(i + 1, 2))

    spans = (pl.ds(0, 3), pl.ds(3, 4))
    low, high = pl.ds(0, shard // 2), pl.ds(shard // 2, shard // 2)

    def place(dz, dy, g, part=None):
        at = lax.rem(zh + dz + NZ, NZ) * NY + lax.rem(yy + dy + NY, NY)
        if part is None:
            return weights.at[at, core, spans[g]]
        return weights.at[at, core, spans[g], part]

    zcopy, zfar, ycopy, yfar, mate = {}, {}, {}, {}, {}

    def z_start(g):
        block = place(0, 0, g)
        zcopy[g] = (send(block, block, z_up), send(block, block, z_down))

    def z_forward(g):
        for copy in zcopy[g]:
            copy.wait_recv()
        one, two = place(-1, 0, g, low), place(1, 0, g, high)
        zfar[g] = (send(one, one, z_up), send(two, two, z_down))

    def z_last(g):
        for copy in zfar[g]:
            copy.wait_recv()

    def y_start(g, dz):
        block = place(dz, 0, g)
        ycopy[g, dz] = (send(block, block, y_up), send(block, block, y_down))

    def y_forward(g, dz):
        for copy in ycopy[g, dz]:
            copy.wait_recv()
        one, two = place(dz, -1, g, low), place(dz, 1, g, high)
        yfar[g, dz] = (send(one, one, y_up), send(two, two, y_down))

    def mate_start(g, dz):
        for copy in yfar[g, dz]:
            copy.wait_recv()
        plane = weights.at[pl.ds(lax.rem(zh + dz + NZ, NZ) * NY, NY), core, spans[g]]
        mate[g, dz] = send(plane, plane, core_mate)

    def mate_wait(g):
        for dz in (0, -1, 1, 2):
            mate[g, dz].wait_recv()

    for load in loads[3:6]:
        load.wait()
    for copy in columns:
        copy.wait_recv()
    z_start(0)
    y_start(0, 0)
    z_start(1)
    y_start(1, 0)

    def ring_next(step, q):
        for d in range(2):
            ring[step, d, q].wait_recv()
            dest = level_of(-step - 1 + 2 * NX if d == 0 else step + 1, 1 - q)
            total = terms[dest, :, col(d)].astype(F32) + partial[d, step - 1, q].astype(F32)
            if step < NX - 1:
                terms[dest, :, col(d)] = total.astype(BF16)
                ring[step + 1, d, q] = ring_send(step + 1, d, q)
            elif q == 0:
                zsend[d] = total.astype(BF16)
                ring["z", d] = send(zsend.at[d], zrecv.at[d], z_mate)
            else:
                own[:, col(d)] = total

    ring_next(1, 0)
    y_forward(0, 0)
    ring_next(1, 1)
    z_forward(0)
    y_start(0, -1)
    y_start(0, 1)
    ring_next(2, 0)
    y_forward(1, 0)
    mate_start(0, 0)
    ring_next(2, 1)
    z_last(0)
    y_start(0, 2)
    ring_next(3, 0)
    y_forward(0, -1)
    y_forward(0, 1)
    z_forward(1)
    y_start(1, -1)
    y_start(1, 1)
    ring_next(3, 1)
    for d in range(2):
        ring["z", d].wait_recv()
        own[:, col(d)] += zrecv[d].astype(F32)

    chunk = 32

    @pl.loop(0, rows // chunk)
    def _(i):
        at = pl.ds(pl.multiple_of(i * chunk, chunk), chunk)
        normed[at] = layer_norm(own[at]).astype(BF16)

    mate_start(0, -1)
    mate_start(0, 1)
    y_forward(0, 2)
    z_last(1)
    y_start(1, 2)
    mate_start(0, 2)
    mate_wait(0)

    def weight(j, start, size):
        return weights[:, :, j, :, pl.ds(start, size)].reshape(width, size)

    def project(j):
        size = half
        for h in range(width // size):
            product = jnp.dot(normed[...], weight(j, h * size, size), preferred_element_type=F32)
            for i in range(size // LANES):
                qkv_s[h * (size // LANES) + i, j] = product[:, i * LANES : (i + 1) * LANES].astype(BF16)

    project(1)
    project(2)
    order = (4, 5, 2, 3, 6, 7, 1)
    kv_copies, q_base = [], None
    for k in order:
        dest = level_of(k // NL, k % NL)
        kv_copies.append(send(qkv_s.at[dest, pl.ds(1, 2)], qkv_r.at[lv, pl.ds(1, 2)], {"level": dest}))
    project(0)
    q_base = used[0]
    for k in range(1, groups):
        dest = level_of(k // NL, k % NL)
        send(qkv_s.at[dest, 0], qkv_r.at[lv, 0], {"level": dest})
    qkv_r[lv] = qkv_s[lv]
    y_forward(1, -1)
    y_forward(1, 1)
    mate_start(1, 0)
    for copy in kv_copies:
        copy.wait_recv()

    head_dim = width // HEADS
    att_base = used[0]
    used[0] += groups - 1

    def attend(src):
        lane = lax.broadcasted_iota(jnp.int32, (rows, LANES), 1)
        query = qkv_r[src, 0].astype(F32) * head_dim ** (-0.5)
        keys = qkv_r[:, 1].reshape(frames, LANES)
        values = qkv_r[:, 2].reshape(frames, LANES)
        mixed = []
        for h in range(LANES // head_dim):
            mine = (lane // head_dim) == h
            masked = jnp.where(mine, query, 0.0).astype(BF16)
            scores = lax.dot_general(masked, keys, (((1,), (1,)), ((), ())), preferred_element_type=F32)
            grown = jnp.exp(scores - jnp.max(scores, axis=-1, keepdims=True))
            total = jnp.sum(grown, axis=-1, keepdims=True)
            mixture = jnp.dot(grown.astype(BF16), values, preferred_element_type=F32) / total
            mixed.append((mine, mixture))
        merged = mixed[0][1]
        for mine, mixture in mixed[1:]:
            merged = jnp.where(mine, mixture, merged)
        return merged.astype(BF16)

    def att_copy(k):
        src = level_of(NX - k // NL, NL - lax.rem(k, NL))
        return src, make(att_s.at[src], att_r.at[:, lane_at], {"level": src}, att_base + k - 1)

    def attend_peers(first_k, last_k):
        @pl.loop(first_k, last_k)
        def _(k):
            src, copy = att_copy(k)
            make(qkv_s.at[src, 0], qkv_r.at[src, 0], {"level": src}, q_base + k - 1).wait_recv()
            att_s[src] = attend(src)
            copy.start()

    attend_peers(1, 4)
    y_forward(1, 2)
    mate_start(1, -1)
    mate_start(1, 1)
    attend_peers(4, groups)
    att_r[:, lane_at] = attend(lv)
    mate_start(1, 2)
    mate_wait(1)

    @pl.loop(1, groups)
    def _(k):
        _, copy = att_copy(k)
        copy.wait_recv()

    attended = lax.dot_general(
        att_r[...], weight(3, 0, width), (((1,), (1,)), ((), ())), preferred_element_type=F32
    )
    after[...] = own[...] + attended

    @pl.loop(0, rows // chunk)
    def _(i):
        at = pl.ds(pl.multiple_of(i * chunk, chunk), chunk)
        normed[at] = layer_norm(after[at]).astype(BF16)

    edge = padded.shape[0] - rows
    edge = edge // 2
    piece = 256
    for h in range(width // piece):
        linear = jnp.dot(normed[...], weight(4, h * piece, piece), preferred_element_type=F32)
        gate = jnp.dot(normed[...], weight(5, h * piece, piece), preferred_element_type=F32)
        value = (linear * jax.nn.sigmoid(gate)).astype(BF16)
        gated[:, pl.ds(h * piece, piece)] = value
        padded[pl.ds(edge, rows), pl.ds(h * piece, piece)] = value.astype(F32)
    tile = halo.shape[1]
    after_me, before_me = lax.rem(lv + 1, groups), lax.rem(lv + groups - 1, groups)
    edges = (
        send(gated.at[pl.ds(rows - tile, tile)], halo.at[0], {"level": after_me}),
        send(gated.at[pl.ds(0, tile)], halo.at[1], {"level": before_me}),
    )

    taps = taps_ref.shape[0]
    reach = taps // 2

    def convolve(start, count):
        conv = jnp.zeros((count, width), F32)
        for t in range(taps):
            conv = conv + padded[pl.ds(edge + start + t - reach, count)] * taps_ref[pl.ds(t, 1)].astype(F32)
        active[pl.ds(start, count)] = (conv * jax.nn.sigmoid(conv)).astype(BF16)

    for start in range(tile, rows - tile, 32):
        convolve(start, 32)
    for copy in edges:
        copy.wait_recv()
    padded[pl.ds(0, edge)] = jnp.where(lv > 0, halo[0, pl.ds(tile - edge, edge)].astype(F32), 0.0)
    padded[pl.ds(edge + rows, edge)] = jnp.where(lv < groups - 1, halo[1, pl.ds(0, edge)].astype(F32), 0.0)
    convolve(0, tile)
    convolve(rows - tile, tile)
    after[...] += jnp.dot(active[...], weight(6, 0, width), preferred_element_type=F32)

    @pl.loop(0, rows // chunk)
    def _(i):
        at = pl.ds(pl.multiple_of(i * chunk, chunk), chunk)
        final[lv, at] = layer_norm(after[at]).astype(BF16)

    stores = []

    def logits(block):
        for h in range(2):
            product = jnp.dot(final[block], head[:, col(h)], preferred_element_type=F32)
            staged[block, :, col(h)] = product.astype(BF16)
        at = pl.ds(pl.multiple_of(block * rows, rows), rows)
        copy = pltpu.make_async_copy(staged.at[block], out_hbm.at[at], store_sem.at[len(stores)])
        copy.start()
        stores.append(copy)

    mine = final.at[lv]
    from_down, from_up, from_mate = send(mine, mine, x_up), send(mine, mine, x_down), send(mine, mine, z_mate)
    top, bottom = pl.ds(0, rows // 2), pl.ds(rows // 2, rows // 2)
    loads[6].wait()
    logits(lv)
    from_down.wait_recv()
    from_up.wait_recv()
    one, two = final.at[level_of(-1, 0), top], final.at[level_of(1, 0), bottom]
    far = (send(one, one, x_up), send(two, two, x_down))
    from_mate.wait_recv()
    mate_block = final.at[level_of(0, 1)]
    mate_down, mate_up = send(mate_block, mate_block, x_up), send(mate_block, mate_block, x_down)
    logits(level_of(-1, 0))
    logits(level_of(1, 0))
    for copy in far:
        copy.wait_recv()
    opposite = final.at[level_of(2, 0)]
    last = send(opposite, opposite, z_mate)
    logits(level_of(0, 1))
    logits(level_of(2, 0))
    mate_down.wait_recv()
    logits(level_of(-1, 1))
    mate_up.wait_recv()
    logits(level_of(1, 1))
    last.wait_recv()
    logits(level_of(2, 1))

    for copy in sent:
        copy.wait_send()

    @pl.loop(1, groups)
    def _(k):
        _, copy = att_copy(k)
        copy.wait_send()

    for copy in stores:
        copy.wait()


def body(
    token_ids,
    decoded_mask,
    levels_done,
    code_tables,
    mask_vectors,
    w_qkv,
    w_out,
    w_expand,
    w_depth,
    w_project,
    level_heads,
):
    frames = token_ids.shape[2]
    width = code_tables.shape[2]
    groups = lax.axis_size("level")
    level = lax.axis_index("level")
    rows = frames // groups
    done = levels_done[0]
    use_token = (level < done) | (level == done) & (decoded_mask[0, 0] == 1)
    sel = jnp.where(use_token, token_ids[0, 0], -1).astype(F32).reshape(groups, rows).T
    shard = w_project.shape[0]
    tile, edge = 16, 8
    vmem = pl.BlockSpec(memory_space=pltpu.VMEM)
    hbm = pl.BlockSpec(memory_space=pl.ANY)
    logits = pl.pallas_call(
        step_kernel,
        out_shape=jax.ShapeDtypeStruct((frames, level_heads.shape[2]), BF16),
        in_specs=[vmem] * 3 + [hbm] * 6,
        out_specs=hbm,
        scratch_shapes=[
            pltpu.VMEM(code_tables.shape[1:], BF16),
            pltpu.VMEM(level_heads.shape[1:], BF16),
            pltpu.VMEM((NZ * NY, NC, 7, shard, width), BF16),
            pltpu.VMEM((groups, rows, width), BF16),
            pltpu.VMEM((2, NX - 1, 2, rows, width // 2), BF16),
            pltpu.VMEM((2, rows, width // 2), BF16),
            pltpu.VMEM((2, rows, width // 2), BF16),
            pltpu.VMEM((rows, width), F32),
            pltpu.VMEM((rows, width), BF16),
            pltpu.VMEM((groups, 3, rows, LANES), BF16),
            pltpu.VMEM((groups, 3, rows, LANES), BF16),
            pltpu.VMEM((groups, rows, LANES), BF16),
            pltpu.VMEM((rows, width), BF16),
            pltpu.VMEM((rows, width), F32),
            pltpu.VMEM((rows, width), BF16),
            pltpu.VMEM((2, tile, width), BF16),
            pltpu.VMEM((rows + 2 * edge, width), F32),
            pltpu.VMEM((rows, width), BF16),
            pltpu.VMEM((groups, rows, width), BF16),
            pltpu.VMEM((groups, rows, width), BF16),
            pltpu.SemaphoreType.DMA((7,)),
            pltpu.SemaphoreType.DMA((groups,)),
            pltpu.SemaphoreType.DMA((COPIES,)),
            pltpu.SemaphoreType.DMA((COPIES,)),
        ],
        compiler_params=pltpu.CompilerParams(
            collective_id=0, has_side_effects=True, vmem_limit_bytes=60 * 1024 * 1024
        ),
    )(
        sel,
        mask_vectors,
        w_depth,
        code_tables[0],
        w_qkv,
        w_out.T,
        w_expand,
        w_project,
        level_heads[0],
    )
    return logits[None, None]


def solution(mesh):
    return jax.shard_map(
        body,
        mesh=mesh,
        in_specs=(
            P("dp", "level", None),
            P("dp", "level", None),
            P("dp"),
            P("level", None, None),
            P("level", None),
            P(None, "dp", "level"),
            P("level", "dp"),
            P("dp", None),
            P(),
            P("dp", None),
            P("level", None, None),
        ),
        out_specs=P("dp", "level", None, None),
        check_vma=False,
    )
```

```python
import jax
import jax.numpy as jnp
from jax import lax
from jax.experimental import pallas as pl
from jax.experimental.pallas import tpu as pltpu
from jax.sharding import PartitionSpec as P

MESH = pl.DeviceIdType.MESH
BF16, F32 = jnp.bfloat16, jnp.float32

HEADS = 16
NZ, NY, NC = 4, 4, 2
NX, NL = 4, 2
LANES = 128
COPIES = 192


def layer_norm(values):
    centered = values - jnp.mean(values, axis=-1, keepdims=True)
    variance = jnp.mean(centered * centered, axis=-1, keepdims=True)
    return centered * lax.rsqrt(variance + 1e-05)


def step_kernel(
    sel_ref,
    fill_ref,
    taps_ref,
    table_hbm,
    wqkv_hbm,
    wout_hbm,
    wexp_hbm,
    wproj_hbm,
    head_hbm,
    out_hbm,
    table,
    head,
    weights,
    terms,
    partial,
    zsend,
    zrecv,
    own,
    normed,
    qkv_s,
    qkv_r,
    att_s,
    att_r,
    after,
    gated,
    halo,
    padded,
    active,
    final,
    staged,
    load_sem,
    store_sem,
    send_sem,
    recv_sem,
):
    groups = NX * NL
    rows, width = own.shape
    frames = rows * groups
    half = width // 2
    shard = weights.shape[3]

    dp = lax.axis_index("dp")
    lv = lax.axis_index("level")
    core = lax.rem(dp, NC)
    yy = lax.rem(dp // NC, NY)
    zh = dp // (NC * NY)
    xx, zl = lv // NL, lax.rem(lv, NL)
    zy = zh * NY + yy

    def level_of(dx, dz):
        return lax.rem(xx + dx + NX, NX) * NL + lax.rem(zl + dz, NL)

    def dp_of(dz, dy, dc):
        return (lax.rem(zh + dz + NZ, NZ) * NY + lax.rem(yy + dy + NY, NY)) * NC + lax.rem(core + dc, NC)

    x_up, x_down, z_mate = {"level": level_of(1, 0)}, {"level": level_of(-1, 0)}, {"level": level_of(0, 1)}
    z_up, z_down = {"dp": dp_of(1, 0, 0)}, {"dp": dp_of(-1, 0, 0)}
    y_up, y_down = {"dp": dp_of(0, 1, 0)}, {"dp": dp_of(0, -1, 0)}
    core_mate = {"dp": dp_of(0, 0, 1)}

    lane_at = pl.ds(pl.multiple_of(lv * LANES, LANES), LANES)
    loads = [
        pltpu.make_async_copy(table_hbm, table, load_sem.at[0]),
        pltpu.make_async_copy(wqkv_hbm, weights.at[zy, core, pl.ds(0, 3), :, lane_at], load_sem.at[1]),
        pltpu.make_async_copy(wout_hbm, weights.at[zy, core, 3, :, lane_at], load_sem.at[2]),
        pltpu.make_async_copy(wexp_hbm.at[:, pl.ds(0, width)], weights.at[zy, core, 4], load_sem.at[3]),
        pltpu.make_async_copy(wexp_hbm.at[:, pl.ds(width, width)], weights.at[zy, core, 5], load_sem.at[4]),
        pltpu.make_async_copy(wproj_hbm, weights.at[zy, core, 6], load_sem.at[5]),
        pltpu.make_async_copy(head_hbm, head, load_sem.at[6]),
    ]
    for load in loads:
        load.start()

    barrier = pltpu.get_barrier_semaphore()
    for k in range(1, groups):
        pl.semaphore_signal(barrier, inc=1, device_id={"level": level_of(k // NL, k % NL)}, device_id_type=MESH)
    for peer in (z_up, z_down, y_up, y_down, core_mate):
        pl.semaphore_signal(barrier, inc=1, device_id=peer, device_id_type=MESH)
    used = [0]
    sent = []

    def make(src, dst, device, index):
        return pltpu.make_async_remote_copy(
            src_ref=src,
            dst_ref=dst,
            send_sem=send_sem.at[index],
            recv_sem=recv_sem.at[index],
            device_id=device,
            device_id_type=MESH,
        )

    def send(src, dst, device):
        copy = make(src, dst, device, used[0])
        used[0] += 1
        copy.start()
        sent.append(copy)
        return copy

    codes = lax.broadcasted_iota(jnp.int32, (rows, table.shape[0]), 1).astype(F32)
    slots = lax.broadcasted_iota(jnp.int32, (rows, groups), 1)

    def term(dx, dz):
        dest = level_of(dx, dz)
        ids = jnp.sum(jnp.where(slots == dest, sel_ref[...], 0.0), axis=1, keepdims=True)
        onehot = jnp.where(ids == codes, 1.0, 0.0).astype(BF16)
        picked = jnp.dot(onehot, table[...], preferred_element_type=F32)
        terms[dest] = jnp.where(ids < 0.0, fill_ref[...].astype(F32), picked).astype(BF16)

    def col(d):
        return pl.ds(d * half, half)

    def ring_send(step, d, q):
        dx = -step if d == 0 else step
        block = terms.at[level_of(dx + NX, 1 - q), :, col(d)]
        return send(block, partial.at[d, step - 1, q], x_up if d == 0 else x_down)

    ring = {}
    loads[0].wait()

    @pl.loop(0, 4)
    def _(i):
        term(2 * lax.rem(i, 2) + NX - 1, 1 - i // 2)

    spans = (pl.ds(1, 2), pl.ds(0, 1), pl.ds(3, 1), pl.ds(4, 3))
    low, high = pl.ds(0, shard // 2), pl.ds(shard // 2, shard // 2)

    def place(dz, dy, g, part=None):
        at = lax.rem(zh + dz + NZ, NZ) * NY + lax.rem(yy + dy + NY, NY)
        if part is None:
            return weights.at[at, core, spans[g]]
        return weights.at[at, core, spans[g], part]

    zcopy, zfar, ycopy, yfar, mate = {}, {}, {}, {}, {}

    def z_start(g):
        block = place(0, 0, g)
        zcopy[g] = (send(block, block, z_up), send(block, block, z_down))

    def z_forward(g):
        for copy in zcopy[g]:
            copy.wait_recv()
        one, two = place(-1, 0, g, low), place(1, 0, g, high)
        zfar[g] = (send(one, one, z_up), send(two, two, z_down))

    def z_last(g):
        for copy in zfar[g]:
            copy.wait_recv()

    def y_start(g, dz):
        block = place(dz, 0, g)
        ycopy[g, dz] = (send(block, block, y_up), send(block, block, y_down))

    def y_forward(g, dz):
        for copy in ycopy[g, dz]:
            copy.wait_recv()
        one, two = place(dz, -1, g, low), place(dz, 1, g, high)
        yfar[g, dz] = (send(one, one, y_up), send(two, two, y_down))

    def mate_start(g, dz):
        for copy in yfar[g, dz]:
            copy.wait_recv()
        plane = weights.at[pl.ds(lax.rem(zh + dz + NZ, NZ) * NY, NY), core, spans[g]]
        mate[g, dz] = send(plane, plane, core_mate)

    def mate_wait(g):
        for dz in (0, -1, 1, 2):
            mate[g, dz].wait_recv()

    def ring_next(step, q):
        for d in range(2):
            ring[step, d, q].wait_recv()
            dest = level_of(-step - 1 + 2 * NX if d == 0 else step + 1, 1 - q)
            total = terms[dest, :, col(d)].astype(F32) + partial[d, step - 1, q].astype(F32)
            if step < NX - 1:
                terms[dest, :, col(d)] = total.astype(BF16)
                ring[step + 1, d, q] = ring_send(step + 1, d, q)
            elif q == 0:
                zsend[d] = total.astype(BF16)
                ring["z", d] = send(zsend.at[d], zrecv.at[d], z_mate)
            else:
                own[:, col(d)] = total

    pl.semaphore_wait(barrier, groups + 4)
    for load in loads[1:6]:
        load.wait()
    first = weights.at[zy, core, pl.ds(0, 4), :, lane_at]
    columns = [send(first, first, {"level": level_of(k // NL, k % NL)}) for k in range(1, groups)]
    for q in range(2):
        for d in range(2):
            ring[1, d, q] = ring_send(1, d, q)
    y_start(3, 0)

    @pl.loop(0, 4)
    def _(i):
        term(2 + 2 * (i // 2), lax.rem(i + 1, 2))

    for copy in columns:
        copy.wait_recv()
    z_start(0)
    y_start(0, 0)
    z_start(1)
    y_start(1, 0)
    ring_next(1, 0)
    y_forward(3, 0)
    y_forward(0, 0)
    ring_next(1, 1)
    z_forward(0)
    y_start(0, -1)
    y_start(0, 1)
    y_forward(1, 0)
    z_forward(1)
    y_start(1, -1)
    y_start(1, 1)
    z_start(2)
    y_start(2, 0)
    z_start(3)
    ring_next(2, 0)
    mate_start(0, 0)
    z_last(0)
    y_start(0, 2)
    z_last(1)
    y_start(1, 2)
    ring_next(2, 1)
    y_forward(0, -1)
    y_forward(0, 1)
    mate_start(1, 0)
    ring_next(3, 0)
    y_forward(1, -1)
    y_forward(1, 1)
    y_forward(0, 2)
    ring_next(3, 1)
    y_forward(1, 2)
    mate_start(0, -1)
    mate_start(0, 1)
    z_forward(2)
    y_start(2, -1)
    y_start(2, 1)
    for d in range(2):
        ring["z", d].wait_recv()
        own[:, col(d)] += zrecv[d].astype(F32)

    chunk = 32

    @pl.loop(0, rows // chunk)
    def _(i):
        at = pl.ds(pl.multiple_of(i * chunk, chunk), chunk)
        normed[at] = layer_norm(own[at]).astype(BF16)

    mate_start(1, -1)
    mate_start(1, 1)
    z_forward(3)
    y_start(3, -1)
    y_start(3, 1)
    mate_start(0, 2)
    mate_start(1, 2)
    mate_wait(0)

    def weight(j, start, size):
        return weights[:, :, j, :, pl.ds(start, size)].reshape(width, size)

    def project(j):
        size = half
        for h in range(width // size):
            product = jnp.dot(normed[...], weight(j, h * size, size), preferred_element_type=F32)
            for i in range(size // LANES):
                qkv_s[h * (size // LANES) + i, j] = product[:, i * LANES : (i + 1) * LANES].astype(BF16)

    project(1)
    project(2)
    order = (4, 5, 2, 3, 6, 7, 1)
    kv_copies, q_base = [], None
    for k in order:
        dest = level_of(k // NL, k % NL)
        kv_copies.append(send(qkv_s.at[dest, pl.ds(1, 2)], qkv_r.at[lv, pl.ds(1, 2)], {"level": dest}))
    mate_wait(1)
    project(0)
    q_base = used[0]
    for k in range(1, groups):
        dest = level_of(k // NL, k % NL)
        send(qkv_s.at[dest, 0], qkv_r.at[lv, 0], {"level": dest})
    qkv_r[lv] = qkv_s[lv]
    z_last(2)
    y_start(2, 2)
    y_forward(2, 0)
    mate_start(3, 0)
    y_forward(2, -1)
    y_forward(2, 1)
    mate_start(2, 0)
    z_last(3)
    y_start(3, 2)
    for copy in kv_copies:
        copy.wait_recv()

    head_dim = width // HEADS
    att_base = used[0]
    used[0] += groups - 1

    def attend(src):
        lane = lax.broadcasted_iota(jnp.int32, (rows, LANES), 1)
        query = qkv_r[src, 0].astype(F32) * head_dim ** (-0.5)
        keys = qkv_r[:, 1].reshape(frames, LANES)
        values = qkv_r[:, 2].reshape(frames, LANES)
        mixed = []
        for h in range(LANES // head_dim):
            mine = (lane // head_dim) == h
            masked = jnp.where(mine, query, 0.0).astype(BF16)
            scores = lax.dot_general(masked, keys, (((1,), (1,)), ((), ())), preferred_element_type=F32)
            grown = jnp.exp(scores - jnp.max(scores, axis=-1, keepdims=True))
            total = jnp.sum(grown, axis=-1, keepdims=True)
            mixture = jnp.dot(grown.astype(BF16), values, preferred_element_type=F32) / total
            mixed.append((mine, mixture))
        merged = mixed[0][1]
        for mine, mixture in mixed[1:]:
            merged = jnp.where(mine, mixture, merged)
        return merged.astype(BF16)

    def att_copy(k):
        src = level_of(NX - k // NL, NL - lax.rem(k, NL))
        return src, make(att_s.at[src], att_r.at[:, lane_at], {"level": src}, att_base + k - 1)

    def attend_peers(first_k, last_k):
        @pl.loop(first_k, last_k)
        def _(k):
            src, copy = att_copy(k)
            make(qkv_s.at[src, 0], qkv_r.at[src, 0], {"level": src}, q_base + k - 1).wait_recv()
            att_s[src] = attend(src)
            copy.start()

    attend_peers(1, 3)
    y_forward(2, 2)
    y_forward(3, -1)
    y_forward(3, 1)
    mate_start(2, -1)
    mate_start(2, 1)
    attend_peers(3, 6)
    y_forward(3, 2)
    mate_start(2, 2)
    mate_start(3, -1)
    mate_start(3, 1)
    attend_peers(6, groups)
    att_r[:, lane_at] = attend(lv)
    mate_start(3, 2)
    mate_wait(2)

    @pl.loop(1, groups)
    def _(k):
        _, copy = att_copy(k)
        copy.wait_recv()

    attended = lax.dot_general(
        att_r[...], weight(3, 0, width), (((1,), (1,)), ((), ())), preferred_element_type=F32
    )
    after[...] = own[...] + attended

    @pl.loop(0, rows // chunk)
    def _(i):
        at = pl.ds(pl.multiple_of(i * chunk, chunk), chunk)
        normed[at] = layer_norm(after[at]).astype(BF16)

    mate_wait(3)
    edge = padded.shape[0] - rows
    edge = edge // 2
    piece = 256
    for h in range(width // piece):
        linear = jnp.dot(normed[...], weight(4, h * piece, piece), preferred_element_type=F32)
        gate = jnp.dot(normed[...], weight(5, h * piece, piece), preferred_element_type=F32)
        value = (linear * jax.nn.sigmoid(gate)).astype(BF16)
        gated[:, pl.ds(h * piece, piece)] = value
        padded[pl.ds(edge, rows), pl.ds(h * piece, piece)] = value.astype(F32)
    tile = halo.shape[1]
    after_me, before_me = lax.rem(lv + 1, groups), lax.rem(lv + groups - 1, groups)
    edges = (
        send(gated.at[pl.ds(rows - tile, tile)], halo.at[0], {"level": after_me}),
        send(gated.at[pl.ds(0, tile)], halo.at[1], {"level": before_me}),
    )

    taps = taps_ref.shape[0]
    reach = taps // 2

    def convolve(start, count):
        conv = jnp.zeros((count, width), F32)
        for t in range(taps):
            conv = conv + padded[pl.ds(edge + start + t - reach, count)] * taps_ref[pl.ds(t, 1)].astype(F32)
        active[pl.ds(start, count)] = (conv * jax.nn.sigmoid(conv)).astype(BF16)

    for start in range(tile, rows - tile, 32):
        convolve(start, 32)
    for copy in edges:
        copy.wait_recv()
    padded[pl.ds(0, edge)] = jnp.where(lv > 0, halo[0, pl.ds(tile - edge, edge)].astype(F32), 0.0)
    padded[pl.ds(edge + rows, edge)] = jnp.where(lv < groups - 1, halo[1, pl.ds(0, edge)].astype(F32), 0.0)
    convolve(0, tile)
    convolve(rows - tile, tile)
    after[...] += jnp.dot(active[...], weight(6, 0, width), preferred_element_type=F32)

    @pl.loop(0, rows // chunk)
    def _(i):
        at = pl.ds(pl.multiple_of(i * chunk, chunk), chunk)
        final[lv, at] = layer_norm(after[at]).astype(BF16)

    stores = []

    def logits(block):
        for h in range(2):
            product = jnp.dot(final[block], head[:, col(h)], preferred_element_type=F32)
            staged[block, :, col(h)] = product.astype(BF16)
        at = pl.ds(pl.multiple_of(block * rows, rows), rows)
        copy = pltpu.make_async_copy(staged.at[block], out_hbm.at[at], store_sem.at[len(stores)])
        copy.start()
        stores.append(copy)

    mine = final.at[lv]
    from_down, from_up, from_mate = send(mine, mine, x_up), send(mine, mine, x_down), send(mine, mine, z_mate)
    top, bottom = pl.ds(0, rows // 2), pl.ds(rows // 2, rows // 2)
    loads[6].wait()
    logits(lv)
    from_down.wait_recv()
    from_up.wait_recv()
    one, two = final.at[level_of(-1, 0), top], final.at[level_of(1, 0), bottom]
    far = (send(one, one, x_up), send(two, two, x_down))
    from_mate.wait_recv()
    mate_block = final.at[level_of(0, 1)]
    mate_down, mate_up = send(mate_block, mate_block, x_up), send(mate_block, mate_block, x_down)
    logits(level_of(-1, 0))
    logits(level_of(1, 0))
    for copy in far:
        copy.wait_recv()
    opposite = final.at[level_of(2, 0)]
    last = send(opposite, opposite, z_mate)
    logits(level_of(0, 1))
    logits(level_of(2, 0))
    mate_down.wait_recv()
    logits(level_of(-1, 1))
    mate_up.wait_recv()
    logits(level_of(1, 1))
    last.wait_recv()
    logits(level_of(2, 1))

    for copy in sent:
        copy.wait_send()

    @pl.loop(1, groups)
    def _(k):
        _, copy = att_copy(k)
        copy.wait_send()

    for copy in stores:
        copy.wait()


def body(
    token_ids,
    decoded_mask,
    levels_done,
    code_tables,
    mask_vectors,
    w_qkv,
    w_out,
    w_expand,
    w_depth,
    w_project,
    level_heads,
):
    frames = token_ids.shape[2]
    width = code_tables.shape[2]
    groups = lax.axis_size("level")
    level = lax.axis_index("level")
    rows = frames // groups
    done = levels_done[0]
    use_token = (level < done) | (level == done) & (decoded_mask[0, 0] == 1)
    sel = jnp.where(use_token, token_ids[0, 0], -1).astype(F32).reshape(groups, rows).T
    shard = w_project.shape[0]
    tile, edge = 16, 8
    vmem = pl.BlockSpec(memory_space=pltpu.VMEM)
    hbm = pl.BlockSpec(memory_space=pl.ANY)
    logits = pl.pallas_call(
        step_kernel,
        out_shape=jax.ShapeDtypeStruct((frames, level_heads.shape[2]), BF16),
        in_specs=[vmem] * 3 + [hbm] * 6,
        out_specs=hbm,
        scratch_shapes=[
            pltpu.VMEM(code_tables.shape[1:], BF16),
            pltpu.VMEM(level_heads.shape[1:], BF16),
            pltpu.VMEM((NZ * NY, NC, 7, shard, width), BF16),
            pltpu.VMEM((groups, rows, width), BF16),
            pltpu.VMEM((2, NX - 1, 2, rows, width // 2), BF16),
            pltpu.VMEM((2, rows, width // 2), BF16),
            pltpu.VMEM((2, rows, width // 2), BF16),
            pltpu.VMEM((rows, width), F32),
            pltpu.VMEM((rows, width), BF16),
            pltpu.VMEM((groups, 3, rows, LANES), BF16),
            pltpu.VMEM((groups, 3, rows, LANES), BF16),
            pltpu.VMEM((groups, rows, LANES), BF16),
            pltpu.VMEM((rows, width), BF16),
            pltpu.VMEM((rows, width), F32),
            pltpu.VMEM((rows, width), BF16),
            pltpu.VMEM((2, tile, width), BF16),
            pltpu.VMEM((rows + 2 * edge, width), F32),
            pltpu.VMEM((rows, width), BF16),
            pltpu.VMEM((groups, rows, width), BF16),
            pltpu.VMEM((groups, rows, width), BF16),
            pltpu.SemaphoreType.DMA((7,)),
            pltpu.SemaphoreType.DMA((groups,)),
            pltpu.SemaphoreType.DMA((COPIES,)),
            pltpu.SemaphoreType.DMA((COPIES,)),
        ],
        compiler_params=pltpu.CompilerParams(
            collective_id=0, has_side_effects=True, vmem_limit_bytes=60 * 1024 * 1024
        ),
    )(
        sel,
        mask_vectors,
        w_depth,
        code_tables[0],
        w_qkv,
        w_out.T,
        w_expand,
        w_project,
        level_heads[0],
    )
    return logits[None, None]


def solution(mesh):
    return jax.shard_map(
        body,
        mesh=mesh,
        in_specs=(
            P("dp", "level", None),
            P("dp", "level", None),
            P("dp"),
            P("level", None, None),
            P("level", None),
            P(None, "dp", "level"),
            P("level", "dp"),
            P("dp", None),
            P(),
            P("dp", None),
            P("level", None, None),
        ),
        out_specs=P("dp", "level", None, None),
        check_vma=False,
    )
```

```python
import jax
import jax.numpy as jnp
from jax import lax
from jax.experimental import pallas as pl
from jax.experimental.pallas import tpu as pltpu
from jax.sharding import PartitionSpec as P

MESH = pl.DeviceIdType.MESH
BF16, F32 = jnp.bfloat16, jnp.float32

HEADS = 16
NZ, NY, NC = 4, 4, 2
NX, NL = 4, 2
LANES = 128
SENDS, ARRIVALS = 40, 92
Q, K, V, OUT, EXPAND, JOIN = range(6)


def layer_norm(values):
    centered = values - jnp.mean(values, axis=-1, keepdims=True)
    variance = jnp.mean(centered * centered, axis=-1, keepdims=True)
    return centered * lax.rsqrt(variance + 1e-05)


def step_kernel(
    sel_ref,
    fill_ref,
    taps_ref,
    table_hbm,
    wqkv_hbm,
    wout_hbm,
    wexp_hbm,
    wproj_hbm,
    head_hbm,
    out,
    table,
    head,
    weights,
    terms,
    partial,
    zsend,
    zrecv,
    own,
    normed,
    qkv_s,
    qkv_r,
    att_s,
    att_r,
    after,
    gated,
    halo,
    padded,
    active,
    final,
    probs,
    sums,
    load_sem,
    send_sem,
    recv_sem,
    att_send,
):
    groups = NX * NL
    rows, width = own.shape
    frames = rows * groups
    half = width // 2
    shard = weights.shape[3]

    dp = lax.axis_index("dp")
    lv = lax.axis_index("level")
    core = lax.rem(dp, NC)
    yy = lax.rem(dp // NC, NY)
    zh = dp // (NC * NY)
    xx, zl = lv // NL, lax.rem(lv, NL)
    zy = zh * NY + yy

    def level_of(dx, dz):
        return lax.rem(xx + dx + NX, NX) * NL + lax.rem(zl + dz, NL)

    def dp_of(dz, dy, dc):
        return (lax.rem(zh + dz + NZ, NZ) * NY + lax.rem(yy + dy + NY, NY)) * NC + lax.rem(core + dc, NC)

    x_up, x_down, z_mate = {"level": level_of(1, 0)}, {"level": level_of(-1, 0)}, {"level": level_of(0, 1)}
    z_up, z_down = {"dp": dp_of(1, 0, 0)}, {"dp": dp_of(-1, 0, 0)}
    y_up, y_down = {"dp": dp_of(0, 1, 0)}, {"dp": dp_of(0, -1, 0)}
    core_mate = {"dp": dp_of(0, 0, 1)}

    lane_at = pl.ds(pl.multiple_of(lv * LANES, LANES), LANES)
    loads = [
        pltpu.make_async_copy(table_hbm, table, load_sem.at[0]),
        pltpu.make_async_copy(wqkv_hbm, weights.at[zy, core, pl.ds(0, 3), :, lane_at], load_sem.at[1]),
        pltpu.make_async_copy(wout_hbm, weights.at[zy, core, 3, :, lane_at], load_sem.at[2]),
        pltpu.make_async_copy(wexp_hbm.at[:, pl.ds(0, width)], weights.at[zy, core, 4], load_sem.at[3]),
        pltpu.make_async_copy(wexp_hbm.at[:, pl.ds(width, width)], weights.at[zy, core, 5], load_sem.at[4]),
        pltpu.make_async_copy(wproj_hbm, weights.at[zy, core, 6], load_sem.at[5]),
        pltpu.make_async_copy(head_hbm, head, load_sem.at[6]),
    ]
    for load in loads:
        load.start()

    barrier = pltpu.get_barrier_semaphore()
    for k in range(1, groups):
        pl.semaphore_signal(barrier, inc=1, device_id={"level": level_of(k // NL, k % NL)}, device_id_type=MESH)
    for peer in (z_up, z_down, y_up, y_down, core_mate):
        pl.semaphore_signal(barrier, inc=1, device_id=peer, device_id_type=MESH)
    sent, arrivals = [], []

    def make(src, dst, device, out_sem, in_sem):
        return pltpu.make_async_remote_copy(
            src_ref=src, dst_ref=dst, send_sem=out_sem, recv_sem=in_sem, device_id=device, device_id_type=MESH
        )

    def arrival():
        arrivals.append(recv_sem.at[len(arrivals)])
        return arrivals[-1]

    def send(src, dst, device, in_sem):
        n = len(sent)
        if n >= SENDS:
            sent[n - SENDS].wait_send()
        copy = make(src, dst, device, send_sem.at[n % SENDS], in_sem)
        copy.start()
        sent.append(copy)

    def await_bytes(ref, in_sem):
        make(ref, ref, core_mate, send_sem.at[0], in_sem).wait_recv()

    codes = lax.broadcasted_iota(jnp.int32, (rows, table.shape[0]), 1).astype(F32)
    slots = lax.broadcasted_iota(jnp.int32, (rows, groups), 1)

    def term(dx, dz):
        dest = level_of(dx, dz)
        ids = jnp.sum(jnp.where(slots == dest, sel_ref[...], 0.0), axis=1, keepdims=True)
        onehot = jnp.where(ids == codes, 1.0, 0.0).astype(BF16)
        picked = jnp.dot(onehot, table[...], preferred_element_type=F32)
        terms[dest] = jnp.where(ids < 0.0, fill_ref[...].astype(F32), picked).astype(BF16)

    def col(d):
        return pl.ds(d * half, half)

    parts = ((1, pl.ds(0, rows)), (0, pl.ds(0, rows // 2)), (0, pl.ds(rows // 2, rows // 2)))

    def ring_send(step, p):
        dz, at = parts[p]
        ring[step, p] = arrival()
        for d in range(2):
            block = terms.at[level_of(NX - step if d == 0 else step, dz), at, col(d)]
            send(block, partial.at[d, step - 1, 1 - dz, at], x_up if d == 0 else x_down, ring[step, p])

    ring = {}
    loads[0].wait()

    @pl.loop(0, 4)
    def _(i):
        term(2 * lax.rem(i, 2) + NX - 1, 1 - i // 2)

    spans = (pl.ds(0, 1), pl.ds(1, 1), pl.ds(2, 1), pl.ds(3, 1), pl.ds(4, 2), pl.ds(6, 1))
    low, high = pl.ds(0, shard // 2), pl.ds(shard // 2, shard // 2)

    def place(dz, dy, g, part=None):
        at = lax.rem(zh + dz + NZ, NZ) * NY + lax.rem(yy + dy + NY, NY)
        if part is None:
            return weights.at[at, core, spans[g]]
        return weights.at[at, core, spans[g], part]

    znear, zfar, ynear, yfar, mate = {}, {}, {}, {}, {}

    def z_start(g):
        block = place(0, 0, g)
        znear[g] = arrival()
        send(block, block, z_up, znear[g])
        send(block, block, z_down, znear[g])

    def z_forward(g):
        await_bytes(weights.at[pl.ds(0, 2), core, spans[g]], znear[g])
        one, two = place(-1, 0, g, low), place(1, 0, g, high)
        zfar[g] = arrival()
        send(one, one, z_up, zfar[g])
        send(two, two, z_down, zfar[g])

    def z_last(g):
        await_bytes(weights.at[0, core, spans[g]], zfar[g])

    def y_start(g, dz):
        block = place(dz, 0, g)
        ynear[g, dz] = arrival()
        send(block, block, y_up, ynear[g, dz])
        send(block, block, y_down, ynear[g, dz])

    def y_forward(g, dz):
        await_bytes(weights.at[pl.ds(0, 2), core, spans[g]], ynear[g, dz])
        one, two = place(dz, -1, g, low), place(dz, 1, g, high)
        yfar[g, dz] = arrival()
        send(one, one, y_up, yfar[g, dz])
        send(two, two, y_down, yfar[g, dz])

    def mate_start(g, dz):
        await_bytes(weights.at[0, core, spans[g]], yfar[g, dz])
        plane = weights.at[pl.ds(lax.rem(zh + dz + NZ, NZ) * NY, NY), core, spans[g]]
        if g not in mate:
            mate[g] = arrival()
        send(plane, plane, core_mate, mate[g])

    def mate_wait(g):
        await_bytes(weights.at[:, core, spans[g]], mate[g])

    z_sem = arrival()

    def ring_next(step, p):
        dz, at = parts[p]
        await_bytes(partial.at[:, step - 1, 1 - dz, at], ring[step, p])
        for d in range(2):
            dest = level_of(2 * NX - step - 1 if d == 0 else step + 1, dz)
            total = terms[dest, at, col(d)].astype(F32) + partial[d, step - 1, 1 - dz, at].astype(F32)
            if step < NX - 1:
                terms[dest, at, col(d)] = total.astype(BF16)
            elif dz == 1:
                zsend[d] = total.astype(BF16)
                send(zsend.at[d], zrecv.at[d], z_mate, z_sem)
            else:
                own[at, col(d)] = total
        if step < NX - 1:
            ring_send(step + 1, p)

    pl.semaphore_wait(barrier, groups + 4)
    for load in loads[1:6]:
        load.wait()

    def columns_start(j, count):
        block = weights.at[zy, core, pl.ds(j, count), :, lane_at]
        sem = arrival()
        for k in range(1, groups):
            send(block, block, {"level": level_of(k // NL, k % NL)}, sem)
        return sem

    def columns_wait(j, count, sem):
        await_bytes(weights.at[zy, core, pl.ds(j, count), :, pl.ds(0, (groups - 1) * LANES)], sem)

    qkv_columns = columns_start(0, 3)
    ring_send(1, 0)
    ring_send(1, 1)
    y_start(EXPAND, 0)
    y_start(JOIN, 0)

    @pl.loop(0, 4)
    def _(i):
        term(2 + 2 * (i // 2), lax.rem(i + 1, 2))

    columns_wait(0, 3, qkv_columns)
    for g in (K, Q, V):
        z_start(g)
        y_start(g, 0)
    ring_next(1, 0)
    ring_send(1, 2)
    y_forward(K, 0)
    y_forward(Q, 0)
    z_forward(K)
    y_start(K, -1)
    y_start(K, 1)
    y_forward(V, 0)
    y_forward(EXPAND, 0)
    y_forward(JOIN, 0)
    z_forward(Q)
    y_start(Q, -1)
    y_start(Q, 1)
    ring_next(2, 0)
    ring_next(1, 1)
    z_forward(V)
    y_start(V, -1)
    y_start(V, 1)
    ring_next(1, 2)
    z_start(EXPAND)
    out_columns = columns_start(3, 1)
    mate_start(K, 0)
    mate_start(Q, 0)
    mate_start(V, 0)
    z_last(K)
    y_start(K, 2)
    z_last(Q)
    y_start(Q, 2)
    y_forward(K, -1)
    y_forward(K, 1)
    z_last(V)
    y_start(V, 2)
    ring_next(3, 0)
    ring_next(2, 1)
    y_forward(Q, -1)
    y_forward(Q, 1)
    ring_next(2, 2)
    z_forward(EXPAND)
    columns_wait(3, 1, out_columns)
    z_start(OUT)
    z_start(JOIN)
    y_forward(V, -1)
    y_forward(V, 1)
    y_forward(K, 2)
    y_forward(Q, 2)
    ring_next(3, 1)
    y_forward(V, 2)
    y_start(EXPAND, -1)
    y_start(EXPAND, 1)
    y_start(OUT, 0)
    mate_start(K, -1)
    mate_start(K, 1)
    mate_start(Q, -1)
    mate_start(Q, 1)
    ring_next(3, 2)
    mate_start(V, -1)
    mate_start(V, 1)
    mate_start(K, 2)
    mate_start(Q, 2)
    mate_start(V, 2)
    await_bytes(zrecv, z_sem)
    for d in range(2):
        own[:, col(d)] += zrecv[d].astype(F32)

    chunk = rows // 2

    @pl.loop(0, rows // chunk)
    def _(i):
        at = pl.ds(pl.multiple_of(i * chunk, chunk), chunk)
        normed[at] = layer_norm(own[at]).astype(BF16)

    mate_wait(K)

    def weight(j, start, size):
        return weights[:, :, j, :, pl.ds(start, size)].reshape(width, size)

    def project(j):
        size = half
        for h in range(width // size):
            product = jnp.dot(normed[...], weight(j, h * size, size), preferred_element_type=F32)
            for i in range(size // LANES):
                qkv_s[h * (size // LANES) + i, j] = product[:, i * LANES : (i + 1) * LANES].astype(BF16)

    def exchange(j, count):
        sem = arrival()
        for k in (4, 5, 2, 3, 6, 7, 1):
            dest = level_of(k // NL, k % NL)
            send(qkv_s.at[dest, pl.ds(j, count)], qkv_r.at[lv, pl.ds(j, count)], {"level": dest}, sem)
        qkv_r[lv, pl.ds(j, count)] = qkv_s[lv, pl.ds(j, count)]
        return sem

    project(1)
    mate_wait(Q)
    project(0)
    qk_sem = exchange(0, 2)
    mate_wait(V)
    project(2)
    v_sem = exchange(2, 1)
    z_last(EXPAND)
    y_start(EXPAND, 2)
    z_forward(OUT)
    y_start(OUT, -1)
    y_start(OUT, 1)
    z_forward(JOIN)
    y_start(JOIN, -1)
    y_start(JOIN, 1)
    mate_start(EXPAND, 0)
    mate_start(JOIN, 0)
    y_forward(EXPAND, -1)
    y_forward(EXPAND, 1)
    y_forward(OUT, 0)
    y_forward(EXPAND, 2)
    await_bytes(qkv_r.at[pl.ds(0, groups - 1), pl.ds(0, 2)], qk_sem)

    head_dim = width // HEADS
    att_sem = arrival()

    heads = LANES // head_dim

    def source(k):
        return level_of(NX - k // NL, NL - lax.rem(k, NL))

    def lane_head():
        return lax.broadcasted_iota(jnp.int32, (rows, LANES), 1) // head_dim

    def score(k):
        src = source(k)
        query = qkv_r[src, 0].astype(F32) * head_dim ** (-0.5)
        keys = qkv_r[:, 1].reshape(frames, LANES)
        total = jnp.zeros((rows, LANES), F32)
        for h in range(heads):
            masked = jnp.where(lane_head() == h, query, 0.0).astype(BF16)
            scores = lax.dot_general(masked, keys, (((1,), (1,)), ((), ())), preferred_element_type=F32)
            grown = jnp.exp(scores - jnp.max(scores, axis=-1, keepdims=True))
            probs[src, h] = grown.astype(BF16)
            total = jnp.where(lane_head() == h, jnp.sum(grown, axis=-1, keepdims=True), total)
        sums[src] = total

    def mix(k):
        src = source(k)
        values = qkv_r[:, 2].reshape(frames, LANES)
        merged = jnp.dot(probs[src, 0], values, preferred_element_type=F32)
        for h in range(1, heads):
            merged = jnp.where(lane_head() == h, jnp.dot(probs[src, h], values, preferred_element_type=F32), merged)
        return (merged / sums[src]).astype(BF16)

    def att_copy(k):
        src = source(k)
        return src, make(att_s.at[src], att_r.at[:, lane_at], {"level": src}, att_send, att_sem)

    def mix_send(k):
        src, copy = att_copy(k)
        att_s[src] = mix(k)
        copy.start()

    @pl.loop(1, 4)
    def _(k):
        score(k)

    z_last(OUT)
    y_start(OUT, 2)
    z_last(JOIN)
    y_start(JOIN, 2)
    await_bytes(qkv_r.at[pl.ds(0, groups - 1), 2], v_sem)

    @pl.loop(1, 4)
    def _(k):
        score(k + 3)
        mix_send(k)

    y_forward(OUT, -1)
    y_forward(OUT, 1)
    y_forward(OUT, 2)
    mate_start(EXPAND, -1)
    mate_start(EXPAND, 1)
    score(7)
    mix_send(4)
    score(0)
    mix_send(5)

    @pl.loop(6, groups)
    def _(k):
        mix_send(k)

    y_forward(JOIN, -1)
    y_forward(JOIN, 1)
    y_forward(JOIN, 2)
    mate_start(OUT, 0)
    mate_start(OUT, -1)
    mate_start(OUT, 1)
    att_r[:, lane_at] = mix(0)
    mate_start(EXPAND, 2)
    mate_start(OUT, 2)
    await_bytes(att_r.at[:, pl.ds(0, (groups - 1) * LANES)], att_sem)
    mate_wait(OUT)

    attended = lax.dot_general(
        att_r[...], weight(3, 0, width), (((1,), (1,)), ((), ())), preferred_element_type=F32
    )
    after[...] = own[...] + attended

    @pl.loop(0, rows // chunk)
    def _(i):
        at = pl.ds(pl.multiple_of(i * chunk, chunk), chunk)
        normed[at] = layer_norm(after[at]).astype(BF16)

    mate_start(JOIN, -1)
    mate_start(JOIN, 1)
    mate_wait(EXPAND)
    edge = padded.shape[0] - rows
    edge = edge // 2
    piece = 256
    for h in range(width // piece):
        linear = jnp.dot(normed[...], weight(4, h * piece, piece), preferred_element_type=F32)
        gate = jnp.dot(normed[...], weight(5, h * piece, piece), preferred_element_type=F32)
        value = (linear * jax.nn.sigmoid(gate)).astype(BF16)
        gated[:, pl.ds(h * piece, piece)] = value
        padded[pl.ds(edge, rows), pl.ds(h * piece, piece)] = value.astype(F32)
    tile = halo.shape[1]
    after_me, before_me = lax.rem(lv + 1, groups), lax.rem(lv + groups - 1, groups)
    mate_start(JOIN, 2)
    edge_sem = arrival()
    send(gated.at[pl.ds(rows - tile, tile)], halo.at[0], {"level": after_me}, edge_sem)
    send(gated.at[pl.ds(0, tile)], halo.at[1], {"level": before_me}, edge_sem)

    taps = taps_ref.shape[0]
    reach = taps // 2

    def convolve(start, count):
        conv = jnp.zeros((count, width), F32)
        for t in range(taps):
            conv = conv + padded[pl.ds(edge + start + t - reach, count)] * taps_ref[pl.ds(t, 1)].astype(F32)
        active[pl.ds(start, count)] = (conv * jax.nn.sigmoid(conv)).astype(BF16)

    for start in range(tile, rows - tile, 32):
        convolve(start, 32)
    await_bytes(halo, edge_sem)
    padded[pl.ds(0, edge)] = jnp.where(lv > 0, halo[0, pl.ds(tile - edge, edge)].astype(F32), 0.0)
    padded[pl.ds(edge + rows, edge)] = jnp.where(lv < groups - 1, halo[1, pl.ds(0, edge)].astype(F32), 0.0)
    convolve(0, tile)
    convolve(rows - tile, tile)
    mate_wait(JOIN)
    after[...] += jnp.dot(active[...], weight(6, 0, width), preferred_element_type=F32)

    @pl.loop(0, rows // chunk)
    def _(i):
        at = pl.ds(pl.multiple_of(i * chunk, chunk), chunk)
        final[lv, at] = layer_norm(after[at]).astype(BF16)

    def logits(block):
        at = pl.ds(pl.multiple_of(block * rows, rows), rows)
        for h in range(2):
            product = jnp.dot(final[block], head[:, col(h)], preferred_element_type=F32)
            out[at, col(h)] = product.astype(BF16)

    mine = final.at[lv]
    side_sem, mate_sem, far_sem, last_sem = arrival(), arrival(), arrival(), arrival()
    down_sem, up_sem = arrival(), arrival()
    send(mine, mine, x_up, side_sem)
    send(mine, mine, x_down, side_sem)
    send(mine, mine, z_mate, mate_sem)
    top, bottom = pl.ds(0, rows // 2), pl.ds(rows // 2, rows // 2)
    loads[6].wait()
    logits(lv)
    await_bytes(final.at[pl.ds(0, 2)], side_sem)
    one, two = final.at[level_of(-1, 0), top], final.at[level_of(1, 0), bottom]
    send(one, one, x_up, far_sem)
    send(two, two, x_down, far_sem)
    await_bytes(final.at[0], mate_sem)
    mate_block = final.at[level_of(0, 1)]
    send(mate_block, mate_block, x_up, down_sem)
    send(mate_block, mate_block, x_down, up_sem)
    logits(level_of(-1, 0))
    logits(level_of(1, 0))
    await_bytes(final.at[0], far_sem)
    opposite = final.at[level_of(2, 0)]
    send(opposite, opposite, z_mate, last_sem)
    logits(level_of(0, 1))
    logits(level_of(2, 0))
    await_bytes(final.at[0], down_sem)
    logits(level_of(-1, 1))
    await_bytes(final.at[0], up_sem)
    logits(level_of(1, 1))
    await_bytes(final.at[0], last_sem)
    logits(level_of(2, 1))

    for copy in sent[-SENDS:]:
        copy.wait_send()
    await_send = make(
        att_s.at[pl.ds(0, groups - 1)], att_s.at[pl.ds(0, groups - 1)], core_mate, att_send, recv_sem.at[0]
    )
    await_send.wait_send()


def body(
    token_ids,
    decoded_mask,
    levels_done,
    code_tables,
    mask_vectors,
    w_qkv,
    w_out,
    w_expand,
    w_depth,
    w_project,
    level_heads,
):
    frames = token_ids.shape[2]
    width = code_tables.shape[2]
    groups = lax.axis_size("level")
    level = lax.axis_index("level")
    rows = frames // groups
    done = levels_done[0]
    use_token = (level < done) | (level == done) & (decoded_mask[0, 0] == 1)
    sel = jnp.where(use_token, token_ids[0, 0], -1).astype(F32).reshape(groups, rows).T
    shard = w_project.shape[0]
    tile, edge = 16, 8
    vmem = pl.BlockSpec(memory_space=pltpu.VMEM)
    hbm = pl.BlockSpec(memory_space=pl.ANY)
    logits = pl.pallas_call(
        step_kernel,
        out_shape=pltpu.VMEM((frames, level_heads.shape[2]), BF16),
        in_specs=[vmem] * 3 + [hbm] * 6,
        out_specs=vmem,
        scratch_shapes=[
            pltpu.VMEM(code_tables.shape[1:], BF16),
            pltpu.VMEM(level_heads.shape[1:], BF16),
            pltpu.VMEM((NZ * NY, NC, 7, shard, width), BF16),
            pltpu.VMEM((groups, rows, width), BF16),
            pltpu.VMEM((2, NX - 1, 2, rows, width // 2), BF16),
            pltpu.VMEM((2, rows, width // 2), BF16),
            pltpu.VMEM((2, rows, width // 2), BF16),
            pltpu.VMEM((rows, width), F32),
            pltpu.VMEM((rows, width), BF16),
            pltpu.VMEM((groups, 3, rows, LANES), BF16),
            pltpu.VMEM((groups, 3, rows, LANES), BF16),
            pltpu.VMEM((groups, rows, LANES), BF16),
            pltpu.VMEM((rows, width), BF16),
            pltpu.VMEM((rows, width), F32),
            pltpu.VMEM((rows, width), BF16),
            pltpu.VMEM((2, tile, width), BF16),
            pltpu.VMEM((rows + 2 * edge, width), F32),
            pltpu.VMEM((rows, width), BF16),
            pltpu.VMEM((groups, rows, width), BF16),
            pltpu.VMEM((groups, LANES * HEADS // width, rows, frames), BF16),
            pltpu.VMEM((groups, rows, LANES), F32),
            pltpu.SemaphoreType.DMA((7,)),
            pltpu.SemaphoreType.DMA((SENDS,)),
            pltpu.SemaphoreType.DMA((ARRIVALS,)),
            pltpu.SemaphoreType.DMA,
        ],
        compiler_params=pltpu.CompilerParams(
            collective_id=0, has_side_effects=True, vmem_limit_bytes=60 * 1024 * 1024
        ),
    )(
        sel,
        mask_vectors,
        w_depth,
        code_tables[0],
        w_qkv,
        w_out.T,
        w_expand,
        w_project,
        level_heads[0],
    )
    return logits[None, None]


def solution(mesh):
    return jax.shard_map(
        body,
        mesh=mesh,
        in_specs=(
            P("dp", "level", None),
            P("dp", "level", None),
            P("dp"),
            P("level", None, None),
            P("level", None),
            P(None, "dp", "level"),
            P("level", "dp"),
            P("dp", None),
            P(),
            P("dp", None),
            P("level", None, None),
        ),
        out_specs=P("dp", "level", None, None),
        check_vma=False,
    )
```

```python
import jax
import jax.numpy as jnp
from jax import lax
from jax.experimental import pallas as pl
from jax.experimental.pallas import tpu as pltpu
from jax.sharding import PartitionSpec as P

MESH = pl.DeviceIdType.MESH
BF16, F32 = jnp.bfloat16, jnp.float32

HEADS = 16
NZ, NY, NC = 4, 4, 2
NX, NL = 4, 2
LANES = 128
EDGE = 16
SENDS, ARRIVALS = 40, 104
Q, K, V, OUT, EXPAND, JOIN = range(6)


def layer_norm(values):
    centered = values - jnp.mean(values, axis=-1, keepdims=True)
    variance = jnp.mean(centered * centered, axis=-1, keepdims=True)
    return centered * lax.rsqrt(variance + 1e-05)


def step_kernel(
    ids_ref,
    mask_ref,
    done_ref,
    fill_ref,
    taps_ref,
    table_hbm,
    wqkv_hbm,
    wout_hbm,
    wexp_hbm,
    wproj_hbm,
    head_hbm,
    out,
    table,
    head,
    id_rows,
    weights,
    terms,
    partial,
    zsend,
    zrecv,
    own,
    normed,
    qkv_s,
    qkv_r,
    att_s,
    att_r,
    after,
    padded,
    active,
    final,
    probs,
    sums,
    load_sem,
    send_sem,
    recv_sem,
    att_send,
):
    groups = NX * NL
    rows, width = active.shape
    frames = rows * groups
    wide = own.shape[0]
    edge = (wide - rows) // 2
    inner = pl.ds(edge, rows)
    half = width // 2
    shard = weights.shape[3]

    dp = lax.axis_index("dp")
    lv = lax.axis_index("level")
    core = lax.rem(dp, NC)
    yy = lax.rem(dp // NC, NY)
    zh = dp // (NC * NY)
    xx, zl = lv // NL, lax.rem(lv, NL)
    zy = zh * NY + yy

    def level_of(dx, dz):
        return lax.rem(xx + dx + NX, NX) * NL + lax.rem(zl + dz, NL)

    def dp_of(dz, dy, dc):
        return (lax.rem(zh + dz + NZ, NZ) * NY + lax.rem(yy + dy + NY, NY)) * NC + lax.rem(core + dc, NC)

    x_up, x_down, z_mate = {"level": level_of(1, 0)}, {"level": level_of(-1, 0)}, {"level": level_of(0, 1)}
    z_up, z_down = {"dp": dp_of(1, 0, 0)}, {"dp": dp_of(-1, 0, 0)}
    y_up, y_down = {"dp": dp_of(0, 1, 0)}, {"dp": dp_of(0, -1, 0)}
    core_mate = {"dp": dp_of(0, 0, 1)}

    lane_at = pl.ds(pl.multiple_of(lv * LANES, LANES), LANES)
    loads = [
        pltpu.make_async_copy(table_hbm, table, load_sem.at[0]),
        pltpu.make_async_copy(wqkv_hbm, weights.at[zy, core, pl.ds(0, 3), :, lane_at], load_sem.at[1]),
        pltpu.make_async_copy(wout_hbm, weights.at[zy, core, 3, :, lane_at], load_sem.at[2]),
        pltpu.make_async_copy(wexp_hbm.at[:, pl.ds(0, width)], weights.at[zy, core, 4], load_sem.at[3]),
        pltpu.make_async_copy(wexp_hbm.at[:, pl.ds(width, width)], weights.at[zy, core, 5], load_sem.at[4]),
        pltpu.make_async_copy(wproj_hbm, weights.at[zy, core, 6], load_sem.at[5]),
        pltpu.make_async_copy(head_hbm, head, load_sem.at[6]),
    ]
    for load in loads:
        load.start()

    barrier = pltpu.get_barrier_semaphore()
    for k in range(1, groups):
        pl.semaphore_signal(barrier, inc=1, device_id={"level": level_of(k // NL, k % NL)}, device_id_type=MESH)
    for peer in (z_up, z_down, y_up, y_down, core_mate):
        pl.semaphore_signal(barrier, inc=1, device_id=peer, device_id_type=MESH)
    sent, arrivals = [], []

    def make(src, dst, device, out_sem, in_sem):
        return pltpu.make_async_remote_copy(
            src_ref=src, dst_ref=dst, send_sem=out_sem, recv_sem=in_sem, device_id=device, device_id_type=MESH
        )

    def arrival():
        arrivals.append(recv_sem.at[len(arrivals)])
        return arrivals[-1]

    def send(src, dst, device, in_sem):
        n = len(sent)
        if n >= SENDS:
            sent[n - SENDS].wait_send()
        copy = make(src, dst, device, send_sem.at[n % SENDS], in_sem)
        copy.start()
        sent.append(copy)

    def await_bytes(ref, in_sem):
        make(ref, ref, core_mate, send_sem.at[0], in_sem).wait_recv()

    done = done_ref[0]
    flags = jnp.where(lv < done, 1, jnp.where(lv == done, mask_ref[...], 0))
    picks = jnp.where(flags == 1, ids_ref[...], -1).astype(F32)
    for i in range(frames // LANES):
        part = jnp.broadcast_to(picks[:, i * LANES : (i + 1) * LANES], (LANES, LANES))
        id_rows[pl.ds(i * LANES, LANES)] = part.T
    codes = lax.broadcasted_iota(jnp.int32, (rows, LANES), 1).astype(F32)
    tiles = table.shape[0] // LANES

    def term(dx, dz):
        dest = level_of(dx, dz)
        ids = id_rows[pl.ds(pl.multiple_of(dest * rows, rows), rows)]
        onehot = jnp.concatenate([jnp.where(ids == codes + i * LANES, 1.0, 0.0).astype(BF16) for i in range(tiles)], axis=1)
        picked = jnp.dot(onehot, table[...], preferred_element_type=F32)
        masked = jnp.concatenate([ids] * (width // LANES), axis=1) < 0.0
        terms[dest] = jnp.where(masked, fill_ref[...].astype(F32), picked).astype(BF16)

    def col(d):
        return pl.ds(d * half, half)

    parts = ((1, pl.ds(0, rows)), (0, pl.ds(0, rows // 2)), (0, pl.ds(rows // 2, rows // 2)))

    def ring_send(step, p):
        dz, at = parts[p]
        ring[step, p] = arrival()
        for d in range(2):
            block = terms.at[level_of(NX - step if d == 0 else step, dz), at, col(d)]
            send(block, partial.at[d, step - 1, 1 - dz, at], x_up if d == 0 else x_down, ring[step, p])

    ring = {}
    loads[0].wait()

    @pl.loop(0, 4)
    def _(i):
        term(2 * lax.rem(i, 2) + NX - 1, 1 - i // 2)

    spans = (pl.ds(0, 1), pl.ds(1, 1), pl.ds(2, 1), pl.ds(3, 1), pl.ds(4, 2), pl.ds(6, 1))
    low, high = pl.ds(0, shard // 2), pl.ds(shard // 2, shard // 2)

    quarter = width // NX
    all_rows, all_lanes = pl.ds(0, shard), pl.ds(0, width)

    def quarter_at(dx):
        return pl.ds(pl.multiple_of(lax.rem(xx + dx + NX, NX) * quarter, LANES), quarter)

    def lanes(g):
        return quarter_at(0) if g == JOIN else all_lanes

    def blocks(at, g, part=all_rows):
        return weights.at[at, core, spans[g], part, lanes(g)]

    def place(dz, dy, g, part=all_rows):
        at = lax.rem(zh + dz + NZ, NZ) * NY + lax.rem(yy + dy + NY, NY)
        return blocks(at, g, part)

    znear, zfar, ynear, yfar, mate = {}, {}, {}, {}, {}

    def z_start(g):
        block = place(0, 0, g)
        znear[g] = arrival()
        send(block, block, z_up, znear[g])
        send(block, block, z_down, znear[g])

    def z_forward(g):
        await_bytes(blocks(pl.ds(0, 2), g), znear[g])
        one, two = place(-1, 0, g, low), place(1, 0, g, high)
        zfar[g] = arrival()
        send(one, one, z_up, zfar[g])
        send(two, two, z_down, zfar[g])

    def z_last(g):
        await_bytes(blocks(0, g), zfar[g])

    def y_start(g, dz):
        block = place(dz, 0, g)
        ynear[g, dz] = arrival()
        send(block, block, y_up, ynear[g, dz])
        send(block, block, y_down, ynear[g, dz])

    def y_forward(g, dz):
        await_bytes(blocks(pl.ds(0, 2), g), ynear[g, dz])
        one, two = place(dz, -1, g, low), place(dz, 1, g, high)
        yfar[g, dz] = arrival()
        send(one, one, y_up, yfar[g, dz])
        send(two, two, y_down, yfar[g, dz])

    def mate_start(g, dz):
        await_bytes(blocks(0, g), yfar[g, dz])
        plane = weights.at[pl.ds(lax.rem(zh + dz + NZ, NZ) * NY, NY), core, spans[g]]
        if g not in mate:
            mate[g] = arrival()
        send(plane, plane, core_mate, mate[g])

    x_sems = []

    def x_start():
        for dz in (0, -1, 1, 2):
            await_bytes(blocks(0, JOIN), yfar[JOIN, dz])
        x_sems.extend([arrival(), arrival()])
        block = weights.at[:, core, 6, :, quarter_at(0)]
        send(block, block, x_up, x_sems[0])
        send(block, block, x_down, x_sems[0])

    def x_forward():
        half_at = NZ * NY // 2
        await_bytes(weights.at[:, core, 6, :, pl.ds(0, 2 * quarter)], x_sems[0])
        one = weights.at[pl.ds(0, half_at), core, 6, :, quarter_at(-1)]
        two = weights.at[pl.ds(half_at, half_at), core, 6, :, quarter_at(1)]
        send(one, one, x_up, x_sems[1])
        send(two, two, x_down, x_sems[1])

    def x_mate():
        await_bytes(weights.at[:, core, 6, :, pl.ds(0, quarter)], x_sems[1])
        mate[JOIN] = arrival()
        block = weights.at[:, core, 6]
        send(block, block, core_mate, mate[JOIN])

    def mate_wait(g):
        await_bytes(weights.at[:, core, spans[g]], mate[g])

    z_sem = arrival()

    def ring_next(step, p):
        dz, at = parts[p]
        await_bytes(partial.at[:, step - 1, 1 - dz, at], ring[step, p])
        for d in range(2):
            dest = level_of(2 * NX - step - 1 if d == 0 else step + 1, dz)
            total = terms[dest, at, col(d)].astype(F32) + partial[d, step - 1, 1 - dz, at].astype(F32)
            if step < NX - 1:
                terms[dest, at, col(d)] = total.astype(BF16)
            elif dz == 1:
                zsend[d] = total.astype(BF16)
                send(zsend.at[d], zrecv.at[d], z_mate, z_sem)
            else:
                own[pl.ds(edge + at.start, at.size), col(d)] = total
        if step < NX - 1:
            ring_send(step + 1, p)

    pl.semaphore_wait(barrier, groups + 4)
    for load in loads[1:6]:
        load.wait()

    def columns_start(j, count):
        block = weights.at[zy, core, pl.ds(j, count), :, lane_at]
        sem = arrival()
        for k in range(1, groups):
            send(block, block, {"level": level_of(k // NL, k % NL)}, sem)
        return sem

    def columns_wait(j, count, sem):
        await_bytes(weights.at[zy, core, pl.ds(j, count), :, pl.ds(0, (groups - 1) * LANES)], sem)

    qkv_columns = columns_start(0, 3)
    ring_send(1, 0)
    out_columns = columns_start(3, 1)
    ring_send(1, 1)
    y_start(EXPAND, 0)
    y_start(JOIN, 0)

    @pl.loop(0, 4)
    def _(i):
        term(2 + 2 * (i // 2), lax.rem(i + 1, 2))

    columns_wait(0, 3, qkv_columns)
    for g in (K, Q, V):
        z_start(g)
        y_start(g, 0)
    z_start(JOIN)
    ring_next(1, 0)
    ring_send(1, 2)
    y_forward(K, 0)
    y_forward(Q, 0)
    z_forward(K)
    y_start(K, -1)
    y_start(K, 1)
    y_forward(V, 0)
    y_forward(JOIN, 0)
    z_forward(Q)
    y_start(Q, -1)
    y_start(Q, 1)
    ring_next(2, 0)
    ring_next(1, 1)
    z_forward(V)
    y_start(V, -1)
    y_start(V, 1)
    z_forward(JOIN)
    y_start(JOIN, -1)
    y_start(JOIN, 1)
    ring_next(1, 2)
    columns_wait(3, 1, out_columns)
    z_start(OUT)
    z_start(EXPAND)
    mate_start(K, 0)
    mate_start(Q, 0)
    mate_start(V, 0)
    z_last(K)
    y_start(K, 2)
    z_last(Q)
    y_start(Q, 2)
    y_forward(K, -1)
    y_forward(K, 1)
    z_last(V)
    y_start(V, 2)
    z_last(JOIN)
    y_start(JOIN, 2)
    ring_next(3, 0)
    ring_next(2, 1)
    y_forward(Q, -1)
    y_forward(Q, 1)
    ring_next(2, 2)
    z_forward(OUT)
    y_forward(V, -1)
    y_forward(V, 1)
    y_forward(JOIN, -1)
    y_forward(JOIN, 1)
    y_forward(K, 2)
    y_forward(Q, 2)
    ring_next(3, 1)
    y_forward(V, 2)
    y_forward(JOIN, 2)
    for dz in (0, -1, 1):
        y_start(OUT, dz)
    y_forward(EXPAND, 0)
    mate_start(K, -1)
    mate_start(K, 1)
    mate_start(Q, -1)
    mate_start(Q, 1)
    ring_next(3, 2)
    x_start()
    mate_start(V, -1)
    mate_start(V, 1)
    mate_start(K, 2)
    mate_start(Q, 2)
    mate_start(V, 2)
    z_forward(EXPAND)
    y_start(EXPAND, -1)
    y_start(EXPAND, 1)
    await_bytes(zrecv, z_sem)
    for d in range(2):
        own[inner, col(d)] += zrecv[d].astype(F32)

    chunk = rows // 2

    @pl.loop(0, rows // chunk)
    def _(i):
        at = pl.ds(pl.multiple_of(edge + i * chunk, 16), chunk)
        normed[at] = layer_norm(own[at]).astype(BF16)

    mate_wait(K)

    def weight(j, start, size):
        return weights[:, :, j, :, pl.ds(start, size)].reshape(width, size)

    def project(j):
        size = half
        for h in range(width // size):
            product = jnp.dot(normed[inner], weight(j, h * size, size), preferred_element_type=F32)
            for i in range(size // LANES):
                qkv_s[h * (size // LANES) + i, j] = product[:, i * LANES : (i + 1) * LANES].astype(BF16)

    def exchange(j, sems):
        for i in range(1, groups):
            k = 3 * i % groups
            dest = level_of(k // NL, k % NL)
            send(qkv_s.at[dest, j], qkv_r.at[lv, j], {"level": dest}, sems[k % len(sems)])
        qkv_r[lv, j] = qkv_s[lv, j]

    def level_of_index(at):
        return lax.rem(at + groups, groups)

    k_sem = arrival()
    project(1)
    exchange(1, (k_sem,))
    mate_wait(Q)
    project(0)
    q_base = len(arrivals)
    exchange(0, [arrival() for _ in range(groups)])
    mate_wait(V)
    project(2)
    v_sem = arrival()
    exchange(2, (v_sem,))
    side = (level_of_index(lv + 1), level_of_index(lv - 1))
    edge_sem = arrival()
    send(own.at[pl.ds(rows, edge)], own.at[pl.ds(0, edge)], {"level": side[0]}, edge_sem)
    send(own.at[pl.ds(edge, edge)], own.at[pl.ds(edge + rows, edge)], {"level": side[1]}, edge_sem)
    z_last(OUT)
    y_start(OUT, 2)
    x_forward()
    for dz in (0, -1, 1):
        y_forward(OUT, dz)
    mate_start(EXPAND, 0)
    z_last(EXPAND)
    y_start(EXPAND, 2)
    y_forward(EXPAND, -1)
    y_forward(EXPAND, 1)
    await_bytes(qkv_r.at[pl.ds(0, groups - 1), 1], k_sem)

    head_dim = width // HEADS
    att_sem, att_low, att_high = arrival(), arrival(), arrival()
    heads = LANES // head_dim

    def source(k):
        return level_of(NX - k // NL, NL - lax.rem(k, NL))

    def lane_head():
        return lax.broadcasted_iota(jnp.int32, (rows, LANES), 1) // head_dim

    def score(k):
        src = source(k)
        query = qkv_r[src, 0].astype(F32) * head_dim ** (-0.5)
        keys = qkv_r[:, 1].reshape(frames, LANES)
        total = jnp.zeros((rows, LANES), F32)
        for h in range(heads):
            masked = jnp.where(lane_head() == h, query, 0.0).astype(BF16)
            scores = lax.dot_general(masked, keys, (((1,), (1,)), ((), ())), preferred_element_type=F32)
            grown = jnp.exp(scores - jnp.max(scores, axis=-1, keepdims=True))
            probs[src, h] = grown.astype(BF16)
            total = jnp.where(lane_head() == h, jnp.sum(grown, axis=-1, keepdims=True), total)
        sums[src] = total

    def mix(k):
        src = source(k)
        values = qkv_r[:, 2].reshape(frames, LANES)
        merged = jnp.dot(probs[src, 0], values, preferred_element_type=F32)
        for h in range(1, heads):
            merged = jnp.where(lane_head() == h, jnp.dot(probs[src, h], values, preferred_element_type=F32), merged)
        return (merged / sums[src]).astype(BF16)

    def send_edges(src, out_low, out_high):
        block = att_s.at[src]
        for rows_at, lands, to, out_sem, in_sem in (
            (pl.ds(rows - edge, edge), pl.ds(0, edge), level_of_index(src + 1), out_low, att_low),
            (pl.ds(0, edge), pl.ds(edge + rows, edge), level_of_index(src - 1), out_high, att_high),
        ):

            @pl.when(to != lv)
            def _():
                make(block.at[rows_at], att_r.at[lands, lane_at], {"level": to}, out_sem, in_sem).start()

            @pl.when(to == lv)
            def _():
                att_r[lands, lane_at] = att_s[src, rows_at]

    def mix_send(k):
        src = source(k)
        att_s[src] = mix(k)
        make(att_s.at[src], att_r.at[inner, lane_at], {"level": src}, att_send.at[0], att_sem).start()
        send_edges(src, att_send.at[1], att_send.at[2])

    def scores_of(first, last):
        @pl.loop(first, last)
        def _(i):
            k = lax.rem(3 * i, groups)
            src = source(k)
            make(qkv_s.at[src, 0], qkv_r.at[src, 0], {"level": src}, send_sem.at[0], recv_sem.at[q_base + k]).wait_recv()
            score(k)

    def mixes_of(first, last):
        @pl.loop(first, last)
        def _(i):
            mix_send(lax.rem(3 * i, groups))

    score(0)
    scores_of(1, 3)
    y_forward(OUT, 2)
    mate_start(OUT, 0)
    scores_of(3, 5)
    mate_start(OUT, -1)
    mate_start(OUT, 1)
    scores_of(5, groups)
    y_forward(EXPAND, 2)
    await_bytes(qkv_r.at[pl.ds(0, groups - 1), 2], v_sem)
    mixes_of(1, 4)
    mate_start(OUT, 2)
    mate_start(EXPAND, -1)
    mate_start(EXPAND, 1)
    x_mate()
    mixes_of(4, groups)
    att_s[lv] = mix(0)
    send_edges(lv, att_send.at[1], att_send.at[2])
    att_r[inner, lane_at] = att_s[lv]
    mate_start(EXPAND, 2)
    others = pl.ds(0, (groups - 1) * LANES)
    await_bytes(att_r.at[inner, others], att_sem)
    await_bytes(att_r.at[pl.ds(0, edge), others], att_low)
    await_bytes(att_r.at[pl.ds(0, edge), others], att_high)
    await_bytes(own.at[pl.ds(0, 2 * edge)], edge_sem)
    mate_wait(OUT)

    attended = lax.dot_general(
        att_r[...], weight(3, 0, width), (((1,), (1,)), ((), ())), preferred_element_type=F32
    )
    after[...] = own[...] + attended

    part = wide // 2

    @pl.loop(0, wide // part)
    def _(i):
        at = pl.ds(pl.multiple_of(i * part, 16), part)
        normed[at] = layer_norm(after[at]).astype(BF16)

    mate_wait(EXPAND)
    piece = 256
    for h in range(width // piece):
        at = pl.ds(h * piece, piece)
        linear = jnp.dot(normed[...], weight(4, h * piece, piece), preferred_element_type=F32)
        gate = jnp.dot(normed[...], weight(5, h * piece, piece), preferred_element_type=F32)
        padded[:, at] = (linear * jax.nn.sigmoid(gate)).astype(BF16).astype(F32)
    padded[pl.ds(0, edge)] = jnp.where(lv > 0, padded[pl.ds(0, edge)], 0.0)
    padded[pl.ds(edge + rows, edge)] = jnp.where(lv < groups - 1, padded[pl.ds(edge + rows, edge)], 0.0)

    taps = taps_ref.shape[0]
    reach = taps // 2

    def convolve(start, count):
        conv = jnp.zeros((count, width), F32)
        for t in range(taps):
            conv = conv + padded[pl.ds(edge + start + t - reach, count)] * taps_ref[pl.ds(t, 1)].astype(F32)
        active[pl.ds(start, count)] = (conv * jax.nn.sigmoid(conv)).astype(BF16)

    for start in range(0, rows, 32):
        convolve(start, 32)
    mate_wait(JOIN)
    after[inner] += jnp.dot(active[...], weight(6, 0, width), preferred_element_type=F32)

    @pl.loop(0, rows // chunk)
    def _(i):
        at = pl.ds(pl.multiple_of(i * chunk, chunk), chunk)
        final[lv, at] = layer_norm(after[pl.ds(pl.multiple_of(edge + i * chunk, 16), chunk)]).astype(BF16)

    def logits(block):
        at = pl.ds(pl.multiple_of(block * rows, rows), rows)
        for h in range(2):
            product = jnp.dot(final[block], head[:, col(h)], preferred_element_type=F32)
            out[at, col(h)] = product.astype(BF16)

    mine = final.at[lv]
    side_sem, mate_sem, far_sem, last_sem = arrival(), arrival(), arrival(), arrival()
    down_sem, up_sem = arrival(), arrival()
    send(mine, mine, x_up, side_sem)
    send(mine, mine, x_down, side_sem)
    send(mine, mine, z_mate, mate_sem)
    top, bottom = pl.ds(0, rows // 2), pl.ds(rows // 2, rows // 2)
    loads[6].wait()
    logits(lv)
    await_bytes(final.at[pl.ds(0, 2)], side_sem)
    one, two = final.at[level_of(-1, 0), top], final.at[level_of(1, 0), bottom]
    send(one, one, x_up, far_sem)
    send(two, two, x_down, far_sem)
    await_bytes(final.at[0], mate_sem)
    mate_block = final.at[level_of(0, 1)]
    send(mate_block, mate_block, x_up, down_sem)
    send(mate_block, mate_block, x_down, up_sem)
    logits(level_of(-1, 0))
    logits(level_of(1, 0))
    await_bytes(final.at[0], far_sem)
    opposite = final.at[level_of(2, 0)]
    send(opposite, opposite, z_mate, last_sem)
    logits(level_of(0, 1))
    logits(level_of(2, 0))
    await_bytes(final.at[0], down_sem)
    logits(level_of(-1, 1))
    await_bytes(final.at[0], up_sem)
    logits(level_of(1, 1))
    await_bytes(final.at[0], last_sem)
    logits(level_of(2, 1))

    for copy in sent[-SENDS:]:
        copy.wait_send()
    for i, ref in enumerate((att_s.at[pl.ds(0, groups - 1)],) + (att_s.at[pl.ds(0, groups - 1), pl.ds(0, edge)],) * 2):
        make(ref, ref, core_mate, att_send.at[i], recv_sem.at[0]).wait_send()


def body(
    token_ids,
    decoded_mask,
    levels_done,
    code_tables,
    mask_vectors,
    w_qkv,
    w_out,
    w_expand,
    w_depth,
    w_project,
    level_heads,
):
    frames = token_ids.shape[2]
    width = code_tables.shape[2]
    groups = lax.axis_size("level")
    rows = frames // groups
    shard = w_project.shape[0]
    wide = rows + 2 * EDGE
    vmem = pl.BlockSpec(memory_space=pltpu.VMEM)
    hbm = pl.BlockSpec(memory_space=pl.ANY)
    logits = pl.pallas_call(
        step_kernel,
        out_shape=pltpu.VMEM((frames, level_heads.shape[2]), BF16),
        in_specs=[vmem] * 2 + [pl.BlockSpec(memory_space=pltpu.SMEM)] + [vmem] * 2 + [hbm] * 6,
        out_specs=vmem,
        scratch_shapes=[
            pltpu.VMEM(code_tables.shape[1:], BF16),
            pltpu.VMEM(level_heads.shape[1:], BF16),
            pltpu.VMEM((frames, LANES), F32),
            pltpu.VMEM((NZ * NY, NC, 7, shard, width), BF16),
            pltpu.VMEM((groups, rows, width), BF16),
            pltpu.VMEM((2, NX - 1, 2, rows, width // 2), BF16),
            pltpu.VMEM((2, rows, width // 2), BF16),
            pltpu.VMEM((2, rows, width // 2), BF16),
            pltpu.VMEM((wide, width), F32),
            pltpu.VMEM((wide, width), BF16),
            pltpu.VMEM((groups, 3, rows, LANES), BF16),
            pltpu.VMEM((groups, 3, rows, LANES), BF16),
            pltpu.VMEM((groups, rows, LANES), BF16),
            pltpu.VMEM((wide, width), BF16),
            pltpu.VMEM((wide, width), F32),
            pltpu.VMEM((wide, width), F32),
            pltpu.VMEM((rows, width), BF16),
            pltpu.VMEM((groups, rows, width), BF16),
            pltpu.VMEM((groups, LANES * HEADS // width, rows, frames), BF16),
            pltpu.VMEM((groups, rows, LANES), F32),
            pltpu.SemaphoreType.DMA((7,)),
            pltpu.SemaphoreType.DMA((SENDS,)),
            pltpu.SemaphoreType.DMA((ARRIVALS,)),
            pltpu.SemaphoreType.DMA((3,)),
        ],
        compiler_params=pltpu.CompilerParams(
            collective_id=0, has_side_effects=True, vmem_limit_bytes=60 * 1024 * 1024
        ),
    )(
        token_ids[0],
        decoded_mask[0],
        levels_done,
        mask_vectors,
        w_depth,
        code_tables[0],
        w_qkv,
        w_out.T,
        w_expand,
        w_project,
        level_heads[0],
    )
    return logits[None, None]


def solution(mesh):
    return jax.shard_map(
        body,
        mesh=mesh,
        in_specs=(
            P("dp", "level", None),
            P("dp", "level", None),
            P("dp"),
            P("level", None, None),
            P("level", None),
            P(None, "dp", "level"),
            P("level", "dp"),
            P("dp", None),
            P(),
            P("dp", None),
            P("level", None, None),
        ),
        out_specs=P("dp", "level", None, None),
        check_vma=False,
    )
```

```python
import jax
import jax.numpy as jnp
from jax import lax
from jax.experimental import pallas as pl
from jax.experimental.pallas import tpu as pltpu
from jax.sharding import PartitionSpec as P

MESH = pl.DeviceIdType.MESH
BF16, F32 = jnp.bfloat16, jnp.float32

HEADS = 16
NZ, NY, NC = 4, 4, 2
NX, NL = 4, 2
LANES = 128
EDGE = 16
SENDS, ARRIVALS = 56, 106
Q, K, V, OUT, EXPAND, JOIN = range(6)


def layer_norm(values):
    centered = values - jnp.mean(values, axis=-1, keepdims=True)
    variance = jnp.mean(centered * centered, axis=-1, keepdims=True)
    return centered * lax.rsqrt(variance + 1e-05)


def step_kernel(
    ids_ref,
    mask_ref,
    done_ref,
    fill_ref,
    taps_ref,
    table_hbm,
    wqkv_hbm,
    wout_hbm,
    wexp_hbm,
    wproj_hbm,
    head_hbm,
    out,
    table,
    head,
    id_rows,
    weights,
    terms,
    partial,
    zsend,
    zrecv,
    own,
    normed,
    qkv_s,
    qkv_r,
    att_s,
    att_r,
    after,
    padded,
    active,
    final,
    probs,
    sums,
    load_sem,
    send_sem,
    recv_sem,
    att_send,
):
    groups = NX * NL
    rows, width = active.shape
    frames = rows * groups
    wide = own.shape[0]
    edge = (wide - rows) // 2
    inner = pl.ds(edge, rows)
    half = width // 2
    shard = weights.shape[3]

    dp = lax.axis_index("dp")
    lv = lax.axis_index("level")
    core = lax.rem(dp, NC)
    yy = lax.rem(dp // NC, NY)
    zh = dp // (NC * NY)
    xx, zl = lv // NL, lax.rem(lv, NL)
    zy = zh * NY + yy

    def level_of(dx, dz):
        return lax.rem(xx + dx + NX, NX) * NL + lax.rem(zl + dz, NL)

    def dp_of(dz, dy, dc):
        return (lax.rem(zh + dz + NZ, NZ) * NY + lax.rem(yy + dy + NY, NY)) * NC + lax.rem(core + dc, NC)

    x_up, x_down, z_mate = {"level": level_of(1, 0)}, {"level": level_of(-1, 0)}, {"level": level_of(0, 1)}
    z_up, z_down = {"dp": dp_of(1, 0, 0)}, {"dp": dp_of(-1, 0, 0)}
    y_up, y_down = {"dp": dp_of(0, 1, 0)}, {"dp": dp_of(0, -1, 0)}
    core_mate = {"dp": dp_of(0, 0, 1)}

    lane_at = pl.ds(pl.multiple_of(lv * LANES, LANES), LANES)
    loads = [
        pltpu.make_async_copy(table_hbm, table, load_sem.at[0]),
        pltpu.make_async_copy(wqkv_hbm, weights.at[zy, core, pl.ds(0, 3), :, lane_at], load_sem.at[1]),
        pltpu.make_async_copy(wout_hbm, weights.at[zy, core, 3, :, lane_at], load_sem.at[2]),
        pltpu.make_async_copy(wexp_hbm.at[:, pl.ds(0, width)], weights.at[zy, core, 4], load_sem.at[3]),
        pltpu.make_async_copy(wexp_hbm.at[:, pl.ds(width, width)], weights.at[zy, core, 5], load_sem.at[4]),
        pltpu.make_async_copy(wproj_hbm, weights.at[zy, core, 6], load_sem.at[5]),
        pltpu.make_async_copy(head_hbm, head, load_sem.at[6]),
    ]
    for load in loads:
        load.start()

    barrier = pltpu.get_barrier_semaphore()
    for k in range(1, groups):
        pl.semaphore_signal(barrier, inc=1, device_id={"level": level_of(k // NL, k % NL)}, device_id_type=MESH)
    for peer in (z_up, z_down, y_up, y_down, core_mate):
        pl.semaphore_signal(barrier, inc=1, device_id=peer, device_id_type=MESH)
    sent, arrivals = [], []

    def make(src, dst, device, out_sem, in_sem):
        return pltpu.make_async_remote_copy(
            src_ref=src, dst_ref=dst, send_sem=out_sem, recv_sem=in_sem, device_id=device, device_id_type=MESH
        )

    def arrival():
        arrivals.append(recv_sem.at[len(arrivals)])
        return arrivals[-1]

    def send(src, dst, device, in_sem):
        n = len(sent)
        if n >= SENDS:
            sent[n - SENDS].wait_send()
        copy = make(src, dst, device, send_sem.at[n % SENDS], in_sem)
        copy.start()
        sent.append(copy)

    def await_bytes(ref, in_sem):
        make(ref, ref, core_mate, send_sem.at[0], in_sem).wait_recv()

    done = done_ref[0]
    flags = jnp.where(lv < done, 1, jnp.where(lv == done, mask_ref[...], 0))
    picks = jnp.where(flags == 1, ids_ref[...], -1).astype(F32)
    for i in range(frames // LANES):
        part = jnp.broadcast_to(picks[:, i * LANES : (i + 1) * LANES], (LANES, LANES))
        id_rows[pl.ds(i * LANES, LANES)] = part.T
    codes = lax.broadcasted_iota(jnp.int32, (rows, LANES), 1).astype(F32)
    tiles = table.shape[0] // LANES

    def term(dx, dz):
        dest = level_of(dx, dz)
        ids = id_rows[pl.ds(pl.multiple_of(dest * rows, rows), rows)]
        onehot = jnp.concatenate([jnp.where(ids == codes + i * LANES, 1.0, 0.0).astype(BF16) for i in range(tiles)], axis=1)
        picked = jnp.dot(onehot, table[...], preferred_element_type=F32)
        masked = jnp.concatenate([ids] * (width // LANES), axis=1) < 0.0
        terms[dest] = jnp.where(masked, fill_ref[...].astype(F32), picked).astype(BF16)

    def col(d):
        return pl.ds(d * half, half)

    parts = ((1, pl.ds(0, rows)), (0, pl.ds(0, rows // 2)), (0, pl.ds(rows // 2, rows // 2)))

    def ring_send(step, p):
        dz, at = parts[p]
        ring[step, p] = arrival()
        for d in range(2):
            block = terms.at[level_of(NX - step if d == 0 else step, dz), at, col(d)]
            send(block, partial.at[d, step - 1, 1 - dz, at], x_up if d == 0 else x_down, ring[step, p])

    ring = {}
    loads[0].wait()

    @pl.loop(0, 4)
    def _(i):
        term(2 * lax.rem(i, 2) + NX - 1, 1 - i // 2)

    spans = (pl.ds(0, 1), pl.ds(1, 1), pl.ds(2, 1), pl.ds(3, 1), pl.ds(4, 2), pl.ds(6, 1))
    low, high = pl.ds(0, shard // 2), pl.ds(shard // 2, shard // 2)

    quarter = width // NX
    all_rows, all_lanes = pl.ds(0, shard), pl.ds(0, width)

    def quarter_at(dx):
        return pl.ds(pl.multiple_of(lax.rem(xx + dx + NX, NX) * quarter, LANES), quarter)

    def lanes(g):
        return quarter_at(0) if g == JOIN else all_lanes

    def blocks(at, g, part=all_rows):
        return weights.at[at, core, spans[g], part, lanes(g)]

    def place(dz, dy, g, part=all_rows):
        at = lax.rem(zh + dz + NZ, NZ) * NY + lax.rem(yy + dy + NY, NY)
        return blocks(at, g, part)

    znear, zfar, ynear, yfar, mate = {}, {}, {}, {}, {}

    def z_start(g):
        block = place(0, 0, g)
        znear[g] = arrival()
        send(block, block, z_up, znear[g])
        send(block, block, z_down, znear[g])

    def z_forward(g):
        await_bytes(blocks(pl.ds(0, 2), g), znear[g])
        one, two = place(-1, 0, g, low), place(1, 0, g, high)
        zfar[g] = arrival()
        send(one, one, z_up, zfar[g])
        send(two, two, z_down, zfar[g])

    def z_last(g):
        await_bytes(blocks(0, g), zfar[g])

    def y_start(g, dz):
        block = place(dz, 0, g)
        ynear[g, dz] = arrival()
        send(block, block, y_up, ynear[g, dz])
        send(block, block, y_down, ynear[g, dz])

    def y_forward(g, dz):
        await_bytes(blocks(pl.ds(0, 2), g), ynear[g, dz])
        one, two = place(dz, -1, g, low), place(dz, 1, g, high)
        yfar[g, dz] = arrival()
        send(one, one, y_up, yfar[g, dz])
        send(two, two, y_down, yfar[g, dz])

    def mate_start(g, dz):
        await_bytes(blocks(0, g), yfar[g, dz])
        plane = weights.at[pl.ds(lax.rem(zh + dz + NZ, NZ) * NY, NY), core, spans[g]]
        if g not in mate:
            mate[g] = arrival()
        send(plane, plane, core_mate, mate[g])

    x_sems = []

    def x_start():
        for dz in (0, -1, 1, 2):
            await_bytes(blocks(0, JOIN), yfar[JOIN, dz])
        x_sems.extend([arrival(), arrival()])
        block = weights.at[:, core, 6, :, quarter_at(0)]
        send(block, block, x_up, x_sems[0])
        send(block, block, x_down, x_sems[0])

    def x_forward():
        half_at = NZ * NY // 2
        await_bytes(weights.at[:, core, 6, :, pl.ds(0, 2 * quarter)], x_sems[0])
        one = weights.at[pl.ds(0, half_at), core, 6, :, quarter_at(-1)]
        two = weights.at[pl.ds(half_at, half_at), core, 6, :, quarter_at(1)]
        send(one, one, x_up, x_sems[1])
        send(two, two, x_down, x_sems[1])

    def x_mate():
        await_bytes(weights.at[:, core, 6, :, pl.ds(0, quarter)], x_sems[1])
        mate[JOIN] = arrival()
        block = weights.at[:, core, 6]
        send(block, block, core_mate, mate[JOIN])

    def mate_wait(g):
        await_bytes(weights.at[:, core, spans[g]], mate[g])

    z_sem = arrival()

    def ring_next(step, p):
        dz, at = parts[p]
        await_bytes(partial.at[:, step - 1, 1 - dz, at], ring[step, p])
        for d in range(2):
            dest = level_of(2 * NX - step - 1 if d == 0 else step + 1, dz)
            total = terms[dest, at, col(d)].astype(F32) + partial[d, step - 1, 1 - dz, at].astype(F32)
            if step < NX - 1:
                terms[dest, at, col(d)] = total.astype(BF16)
            elif dz == 1:
                zsend[d] = total.astype(BF16)
                send(zsend.at[d], zrecv.at[d], z_mate, z_sem)
            else:
                own[pl.ds(edge + at.start, at.size), col(d)] = total
        if step < NX - 1:
            ring_send(step + 1, p)

    pl.semaphore_wait(barrier, groups + 4)
    for load in loads[1:6]:
        load.wait()

    def columns_start(j, count):
        block = weights.at[zy, core, pl.ds(j, count), :, lane_at]
        sem = arrival()
        for k in range(1, groups):
            send(block, block, {"level": level_of(k // NL, k % NL)}, sem)
        return sem

    def columns_wait(j, count, sem):
        await_bytes(weights.at[zy, core, pl.ds(j, count), :, pl.ds(0, (groups - 1) * LANES)], sem)

    qkv_columns = columns_start(0, 3)
    ring_send(1, 0)
    out_columns = columns_start(3, 1)
    ring_send(1, 1)
    y_start(EXPAND, 0)
    y_start(JOIN, 0)

    @pl.loop(0, 4)
    def _(i):
        term(2 + 2 * (i // 2), lax.rem(i + 1, 2))

    columns_wait(0, 3, qkv_columns)
    for g in (K, Q):
        z_start(g)
        y_start(g, 0)
    z_start(JOIN)
    z_start(V)
    y_start(V, 0)
    ring_next(1, 0)
    ring_send(1, 2)
    y_forward(K, 0)
    y_forward(Q, 0)
    z_forward(K)
    y_start(K, -1)
    y_start(K, 1)
    y_forward(V, 0)
    y_forward(JOIN, 0)
    z_forward(Q)
    y_start(Q, -1)
    y_start(Q, 1)
    ring_next(2, 0)
    ring_next(1, 1)
    z_forward(JOIN)
    y_start(JOIN, -1)
    y_start(JOIN, 1)
    z_forward(V)
    y_start(V, -1)
    y_start(V, 1)
    ring_next(1, 2)
    columns_wait(3, 1, out_columns)
    z_start(OUT)
    mate_start(K, 0)
    mate_start(Q, 0)
    mate_start(V, 0)
    z_last(K)
    y_start(K, 2)
    z_last(Q)
    y_start(Q, 2)
    y_forward(K, -1)
    y_forward(K, 1)
    z_last(JOIN)
    y_start(JOIN, 2)
    z_last(V)
    y_start(V, 2)
    ring_next(3, 0)
    z_start(EXPAND)
    ring_next(2, 1)
    y_forward(Q, -1)
    y_forward(Q, 1)
    ring_next(2, 2)
    z_forward(OUT)
    y_forward(JOIN, -1)
    y_forward(JOIN, 1)
    y_forward(V, -1)
    y_forward(V, 1)
    y_forward(K, 2)
    y_forward(Q, 2)
    ring_next(3, 1)
    y_forward(JOIN, 2)
    y_forward(V, 2)
    for dz in (0, -1, 1):
        y_start(OUT, dz)
    y_forward(EXPAND, 0)
    mate_start(K, -1)
    mate_start(K, 1)
    mate_start(Q, -1)
    mate_start(Q, 1)
    ring_next(3, 2)
    x_start()
    mate_start(V, -1)
    mate_start(V, 1)
    mate_start(K, 2)
    mate_start(Q, 2)
    mate_start(V, 2)
    await_bytes(zrecv, z_sem)
    for d in range(2):
        own[inner, col(d)] += zrecv[d].astype(F32)

    chunk = rows // 2

    @pl.loop(0, rows // chunk)
    def _(i):
        at = pl.ds(pl.multiple_of(edge + i * chunk, 16), chunk)
        normed[at] = layer_norm(own[at]).astype(BF16)

    mate_wait(K)

    def weight(j, start, size):
        return weights[:, :, j, :, pl.ds(start, size)].reshape(width, size)

    def project(j):
        size = half
        for h in range(width // size):
            product = jnp.dot(normed[inner], weight(j, h * size, size), preferred_element_type=F32)
            for i in range(size // LANES):
                qkv_s[h * (size // LANES) + i, j] = product[:, i * LANES : (i + 1) * LANES].astype(BF16)

    def exchange(j, sems):
        for i in range(1, groups):
            k = 3 * i % groups
            dest = level_of(k // NL, k % NL)
            send(qkv_s.at[dest, j], qkv_r.at[lv, j], {"level": dest}, sems[k % len(sems)])
        qkv_r[lv, j] = qkv_s[lv, j]

    def level_of_index(at):
        return lax.rem(at + groups, groups)

    k_sem = arrival()
    project(1)
    exchange(1, (k_sem,))
    z_forward(EXPAND)
    y_start(EXPAND, -1)
    y_start(EXPAND, 1)
    mate_wait(Q)
    project(0)
    q_base = len(arrivals)
    exchange(0, [arrival() for _ in range(groups)])
    mate_wait(V)
    project(2)
    v_sem = arrival()
    exchange(2, (v_sem,))
    side = (level_of_index(lv + 1), level_of_index(lv - 1))
    edge_sem = arrival()
    send(own.at[pl.ds(rows, edge)], own.at[pl.ds(0, edge)], {"level": side[0]}, edge_sem)
    send(own.at[pl.ds(edge, edge)], own.at[pl.ds(edge + rows, edge)], {"level": side[1]}, edge_sem)
    z_last(OUT)
    y_start(OUT, 2)
    for dz in (0, -1, 1):
        y_forward(OUT, dz)
    await_bytes(qkv_r.at[pl.ds(0, groups - 1), 1], k_sem)

    head_dim = width // HEADS
    att_sem, att_low, att_high = arrival(), arrival(), arrival()
    heads = LANES // head_dim

    def source(k):
        return level_of(NX - k // NL, NL - lax.rem(k, NL))

    def lane_head():
        return lax.broadcasted_iota(jnp.int32, (rows, LANES), 1) // head_dim

    def score(k):
        src = source(k)
        query = qkv_r[src, 0].astype(F32) * head_dim ** (-0.5)
        keys = qkv_r[:, 1].reshape(frames, LANES)
        total = jnp.zeros((rows, LANES), F32)
        for h in range(heads):
            masked = jnp.where(lane_head() == h, query, 0.0).astype(BF16)
            scores = lax.dot_general(masked, keys, (((1,), (1,)), ((), ())), preferred_element_type=F32)
            grown = jnp.exp(scores - jnp.max(scores, axis=-1, keepdims=True))
            probs[src, h] = grown.astype(BF16)
            total = jnp.where(lane_head() == h, jnp.sum(grown, axis=-1, keepdims=True), total)
        sums[src] = total

    def mix(k):
        src = source(k)
        values = qkv_r[:, 2].reshape(frames, LANES)
        merged = jnp.dot(probs[src, 0], values, preferred_element_type=F32)
        for h in range(1, heads):
            merged = jnp.where(lane_head() == h, jnp.dot(probs[src, h], values, preferred_element_type=F32), merged)
        return (merged / sums[src]).astype(BF16)

    def send_edges(src, out_low, out_high):
        block = att_s.at[src]
        for rows_at, lands, to, out_sem, in_sem in (
            (pl.ds(rows - edge, edge), pl.ds(0, edge), level_of_index(src + 1), out_low, att_low),
            (pl.ds(0, edge), pl.ds(edge + rows, edge), level_of_index(src - 1), out_high, att_high),
        ):

            @pl.when(to != lv)
            def _():
                make(block.at[rows_at], att_r.at[lands, lane_at], {"level": to}, out_sem, in_sem).start()

            @pl.when(to == lv)
            def _():
                att_r[lands, lane_at] = att_s[src, rows_at]

    def mix_send(k):
        src = source(k)
        att_s[src] = mix(k)
        make(att_s.at[src], att_r.at[inner, lane_at], {"level": src}, att_send.at[0], att_sem).start()
        send_edges(src, att_send.at[1], att_send.at[2])

    def scores_of(first, last):
        @pl.loop(first, last)
        def _(i):
            k = lax.rem(3 * i, groups)
            src = source(k)
            make(qkv_s.at[src, 0], qkv_r.at[src, 0], {"level": src}, send_sem.at[0], recv_sem.at[q_base + k]).wait_recv()
            score(k)

    def mixes_of(first, last):
        @pl.loop(first, last)
        def _(i):
            mix_send(lax.rem(3 * i, groups))

    score(0)
    scores_of(1, 3)
    x_forward()
    mate_start(EXPAND, 0)
    y_forward(OUT, 2)
    mate_start(OUT, 0)
    y_forward(EXPAND, -1)
    y_forward(EXPAND, 1)
    scores_of(3, 5)
    mate_start(OUT, -1)
    mate_start(OUT, 1)
    z_last(EXPAND)
    y_start(EXPAND, 2)
    scores_of(5, groups)
    await_bytes(qkv_r.at[pl.ds(0, groups - 1), 2], v_sem)
    mixes_of(1, 4)
    mate_start(OUT, 2)
    y_forward(EXPAND, 2)
    mate_start(EXPAND, -1)
    mate_start(EXPAND, 1)
    x_mate()
    mixes_of(4, groups)
    att_s[lv] = mix(0)
    send_edges(lv, att_send.at[1], att_send.at[2])
    att_r[inner, lane_at] = att_s[lv]
    mate_start(EXPAND, 2)
    others = pl.ds(0, (groups - 1) * LANES)
    await_bytes(att_r.at[inner, others], att_sem)
    await_bytes(att_r.at[pl.ds(0, edge), others], att_low)
    await_bytes(att_r.at[pl.ds(0, edge), others], att_high)
    await_bytes(own.at[pl.ds(0, 2 * edge)], edge_sem)
    mate_wait(OUT)

    attended = lax.dot_general(
        att_r[...], weight(3, 0, width), (((1,), (1,)), ((), ())), preferred_element_type=F32
    )
    after[...] = own[...] + attended

    part = wide // 2

    @pl.loop(0, wide // part)
    def _(i):
        at = pl.ds(pl.multiple_of(i * part, 16), part)
        normed[at] = layer_norm(after[at]).astype(BF16)

    mate_wait(EXPAND)
    piece = 256
    for h in range(width // piece):
        at = pl.ds(h * piece, piece)
        linear = jnp.dot(normed[...], weight(4, h * piece, piece), preferred_element_type=F32)
        gate = jnp.dot(normed[...], weight(5, h * piece, piece), preferred_element_type=F32)
        padded[:, at] = (linear * jax.nn.sigmoid(gate)).astype(BF16).astype(F32)
    padded[pl.ds(0, edge)] = jnp.where(lv > 0, padded[pl.ds(0, edge)], 0.0)
    padded[pl.ds(edge + rows, edge)] = jnp.where(lv < groups - 1, padded[pl.ds(edge + rows, edge)], 0.0)

    taps = taps_ref.shape[0]
    reach = taps // 2

    def convolve(start, count):
        conv = jnp.zeros((count, width), F32)
        for t in range(taps):
            conv = conv + padded[pl.ds(edge + start + t - reach, count)] * taps_ref[pl.ds(t, 1)].astype(F32)
        active[pl.ds(start, count)] = (conv * jax.nn.sigmoid(conv)).astype(BF16)

    mate_wait(JOIN)

    part = rows // 2
    share = part // 6 // EDGE * EDGE
    side_sems, mate_sems, far_sems, last_sems, tail_sems, cross_sems = ([arrival(), arrival()] for _ in range(6))

    for n in range(2):
        at, wide_at = pl.ds(n * part, part), pl.ds(edge + n * part, part)
        for start in range(n * part, (n + 1) * part, 32):
            convolve(start, 32)
        after[wide_at] += jnp.dot(active[at], weight(6, 0, width), preferred_element_type=F32)
        final[lv, at] = layer_norm(after[wide_at]).astype(BF16)
        mine = final.at[lv, at]
        send(mine, mine, x_up, side_sems[n])
        send(mine, mine, x_down, side_sems[n])
        send(mine, mine, z_mate, mate_sems[n])

    def logits(block, start=0, count=rows):
        at = pl.ds(pl.multiple_of(block * rows + start, 32), count)
        states = final[block, pl.ds(start, count)]
        for h in range(2):
            product = jnp.dot(states, head[:, col(h)], preferred_element_type=F32)
            out[at, col(h)] = product.astype(BF16)

    loads[6].wait()
    logits(lv)
    for n in range(2):
        start, middle = n * part, n * part + part // 2
        await_bytes(final.at[pl.ds(0, 2), pl.ds(0, part)], side_sems[n])
        one = final.at[level_of(-1, 0), pl.ds(start, part // 2)]
        two = final.at[level_of(1, 0), pl.ds(middle, part // 2)]
        send(one, one, x_up, far_sems[n])
        send(two, two, x_down, far_sems[n])
        for dx in (-1, 1):
            tail = final.at[level_of(dx, 0), pl.ds(start + part - share, share)]
            send(tail, tail, z_mate, tail_sems[n])
    for n in range(2):
        await_bytes(final.at[0, pl.ds(0, part)], mate_sems[n])
        block = final.at[level_of(0, 1), pl.ds(n * part, part - share)]
        send(block, block, x_up, cross_sems[n])
        send(block, block, x_down, cross_sems[n])
    logits(level_of(-1, 0))
    logits(level_of(1, 0))
    for n in range(2):
        await_bytes(final.at[0, pl.ds(0, part)], far_sems[n])
        block = final.at[level_of(2, 0), pl.ds(n * part, part)]
        send(block, block, z_mate, last_sems[n])
        logits(level_of(2 * n, 1 - n))
    for n in range(2):
        await_bytes(final.at[pl.ds(0, 2), pl.ds(0, part - share)], cross_sems[n])
        await_bytes(final.at[pl.ds(0, 2), pl.ds(0, share)], tail_sems[n])
        logits(level_of(-1, 1), n * part, part)
        logits(level_of(1, 1), n * part, part)
        await_bytes(final.at[0, pl.ds(0, part)], last_sems[n])
        logits(level_of(2, 1), n * part, part)

    for copy in sent[-SENDS:]:
        copy.wait_send()
    for i, ref in enumerate((att_s.at[pl.ds(0, groups - 1)],) + (att_s.at[pl.ds(0, groups - 1), pl.ds(0, edge)],) * 2):
        make(ref, ref, core_mate, att_send.at[i], recv_sem.at[0]).wait_send()


def body(
    token_ids,
    decoded_mask,
    levels_done,
    code_tables,
    mask_vectors,
    w_qkv,
    w_out,
    w_expand,
    w_depth,
    w_project,
    level_heads,
):
    frames = token_ids.shape[2]
    width = code_tables.shape[2]
    groups = lax.axis_size("level")
    rows = frames // groups
    shard = w_project.shape[0]
    wide = rows + 2 * EDGE
    vmem = pl.BlockSpec(memory_space=pltpu.VMEM)
    hbm = pl.BlockSpec(memory_space=pl.ANY)
    logits = pl.pallas_call(
        step_kernel,
        out_shape=pltpu.VMEM((frames, level_heads.shape[2]), BF16),
        in_specs=[vmem] * 2 + [pl.BlockSpec(memory_space=pltpu.SMEM)] + [vmem] * 2 + [hbm] * 6,
        out_specs=vmem,
        scratch_shapes=[
            pltpu.VMEM(code_tables.shape[1:], BF16),
            pltpu.VMEM(level_heads.shape[1:], BF16),
            pltpu.VMEM((frames, LANES), F32),
            pltpu.VMEM((NZ * NY, NC, 7, shard, width), BF16),
            pltpu.VMEM((groups, rows, width), BF16),
            pltpu.VMEM((2, NX - 1, 2, rows, width // 2), BF16),
            pltpu.VMEM((2, rows, width // 2), BF16),
            pltpu.VMEM((2, rows, width // 2), BF16),
            pltpu.VMEM((wide, width), F32),
            pltpu.VMEM((wide, width), BF16),
            pltpu.VMEM((groups, 3, rows, LANES), BF16),
            pltpu.VMEM((groups, 3, rows, LANES), BF16),
            pltpu.VMEM((groups, rows, LANES), BF16),
            pltpu.VMEM((wide, width), BF16),
            pltpu.VMEM((wide, width), F32),
            pltpu.VMEM((wide, width), F32),
            pltpu.VMEM((rows, width), BF16),
            pltpu.VMEM((groups, rows, width), BF16),
            pltpu.VMEM((groups, LANES * HEADS // width, rows, frames), BF16),
            pltpu.VMEM((groups, rows, LANES), F32),
            pltpu.SemaphoreType.DMA((7,)),
            pltpu.SemaphoreType.DMA((SENDS,)),
            pltpu.SemaphoreType.DMA((ARRIVALS,)),
            pltpu.SemaphoreType.DMA((3,)),
        ],
        compiler_params=pltpu.CompilerParams(
            collective_id=0, has_side_effects=True, vmem_limit_bytes=60 * 1024 * 1024
        ),
    )(
        token_ids[0],
        decoded_mask[0],
        levels_done,
        mask_vectors,
        w_depth,
        code_tables[0],
        w_qkv,
        w_out.T,
        w_expand,
        w_project,
        level_heads[0],
    )
    return logits[None, None]


def solution(mesh):
    return jax.shard_map(
        body,
        mesh=mesh,
        in_specs=(
            P("dp", "level", None),
            P("dp", "level", None),
            P("dp"),
            P("level", None, None),
            P("level", None),
            P(None, "dp", "level"),
            P("level", "dp"),
            P("dp", None),
            P(),
            P("dp", None),
            P("level", None, None),
        ),
        out_specs=P("dp", "level", None, None),
        check_vma=False,
    )
```

```python
import jax
import jax.numpy as jnp
from jax import lax
from jax.experimental import pallas as pl
from jax.experimental.pallas import tpu as pltpu
from jax.sharding import PartitionSpec as P

MESH = pl.DeviceIdType.MESH
BF16, F32 = jnp.bfloat16, jnp.float32

HEADS = 16
NZ, NY, NC = 4, 4, 2
NX, NL = 4, 2
LANES = 128
EDGE = 16
SENDS, ARRIVALS = 56, 106
Q, K, V, OUT, EXPAND, JOIN = range(6)


def layer_norm(values):
    centered = values - jnp.mean(values, axis=-1, keepdims=True)
    variance = jnp.mean(centered * centered, axis=-1, keepdims=True)
    return centered * lax.rsqrt(variance + 1e-05)


def step_kernel(
    ids_ref,
    mask_ref,
    done_ref,
    fill_ref,
    taps_ref,
    table_hbm,
    wqkv_hbm,
    wout_hbm,
    wexp_hbm,
    wproj_hbm,
    head_hbm,
    out,
    table,
    head,
    id_rows,
    weights,
    terms,
    partial,
    zsend,
    zrecv,
    own,
    normed,
    qkv_s,
    qkv_r,
    att_s,
    att_r,
    after,
    padded,
    active,
    final,
    probs,
    sums,
    load_sem,
    send_sem,
    recv_sem,
    att_send,
):
    groups = NX * NL
    rows, width = active.shape
    frames = rows * groups
    wide = own.shape[0]
    edge = (wide - rows) // 2
    inner = pl.ds(edge, rows)
    half = width // 2
    shard = weights.shape[3]

    dp = lax.axis_index("dp")
    lv = lax.axis_index("level")
    core = lax.rem(dp, NC)
    yy = lax.rem(dp // NC, NY)
    zh = dp // (NC * NY)
    xx, zl = lv // NL, lax.rem(lv, NL)
    zy = zh * NY + yy

    def level_of(dx, dz):
        return lax.rem(xx + dx + NX, NX) * NL + lax.rem(zl + dz, NL)

    def dp_of(dz, dy, dc):
        return (lax.rem(zh + dz + NZ, NZ) * NY + lax.rem(yy + dy + NY, NY)) * NC + lax.rem(core + dc, NC)

    x_up, x_down, z_mate = {"level": level_of(1, 0)}, {"level": level_of(-1, 0)}, {"level": level_of(0, 1)}
    z_up, z_down = {"dp": dp_of(1, 0, 0)}, {"dp": dp_of(-1, 0, 0)}
    y_up, y_down = {"dp": dp_of(0, 1, 0)}, {"dp": dp_of(0, -1, 0)}
    core_mate = {"dp": dp_of(0, 0, 1)}

    lane_at = pl.ds(pl.multiple_of(lv * LANES, LANES), LANES)
    loads = [
        pltpu.make_async_copy(table_hbm, table, load_sem.at[0]),
        pltpu.make_async_copy(wqkv_hbm, weights.at[zy, core, pl.ds(0, 3), :, lane_at], load_sem.at[1]),
        pltpu.make_async_copy(wout_hbm, weights.at[zy, core, 3, :, lane_at], load_sem.at[2]),
        pltpu.make_async_copy(wexp_hbm.at[:, pl.ds(0, width)], weights.at[zy, core, 4], load_sem.at[3]),
        pltpu.make_async_copy(wexp_hbm.at[:, pl.ds(width, width)], weights.at[zy, core, 5], load_sem.at[4]),
        pltpu.make_async_copy(wproj_hbm, weights.at[zy, core, 6], load_sem.at[5]),
        pltpu.make_async_copy(head_hbm, head, load_sem.at[6]),
    ]
    for load in loads:
        load.start()

    barrier = pltpu.get_barrier_semaphore()
    for k in range(1, groups):
        pl.semaphore_signal(barrier, inc=1, device_id={"level": level_of(k // NL, k % NL)}, device_id_type=MESH)
    for peer in (z_up, z_down, y_up, y_down, core_mate):
        pl.semaphore_signal(barrier, inc=1, device_id=peer, device_id_type=MESH)
    sent, arrivals = [], []

    def make(src, dst, device, out_sem, in_sem):
        return pltpu.make_async_remote_copy(
            src_ref=src, dst_ref=dst, send_sem=out_sem, recv_sem=in_sem, device_id=device, device_id_type=MESH
        )

    def arrival():
        arrivals.append(recv_sem.at[len(arrivals)])
        return arrivals[-1]

    def send(src, dst, device, in_sem):
        n = len(sent)
        if n >= SENDS:
            sent[n - SENDS].wait_send()
        copy = make(src, dst, device, send_sem.at[n % SENDS], in_sem)
        copy.start()
        sent.append(copy)

    def await_bytes(ref, in_sem):
        make(ref, ref, core_mate, send_sem.at[0], in_sem).wait_recv()

    done = done_ref[0]
    flags = jnp.where(lv < done, 1, jnp.where(lv == done, mask_ref[...], 0))
    picks = jnp.where(flags == 1, ids_ref[...], -1).astype(F32)
    for i in range(frames // LANES):
        part = jnp.broadcast_to(picks[:, i * LANES : (i + 1) * LANES], (LANES, LANES))
        id_rows[pl.ds(i * LANES, LANES)] = part.T
    codes = lax.broadcasted_iota(jnp.int32, (rows, LANES), 1).astype(F32)
    tiles = table.shape[0] // LANES

    def term(dx, dz):
        dest = level_of(dx, dz)
        ids = id_rows[pl.ds(pl.multiple_of(dest * rows, rows), rows)]
        onehot = jnp.concatenate([jnp.where(ids == codes + i * LANES, 1.0, 0.0).astype(BF16) for i in range(tiles)], axis=1)
        picked = jnp.dot(onehot, table[...], preferred_element_type=F32)
        masked = jnp.concatenate([ids] * (width // LANES), axis=1) < 0.0
        terms[dest] = jnp.where(masked, fill_ref[...].astype(F32), picked).astype(BF16)

    def col(d):
        return pl.ds(d * half, half)

    parts = ((1, pl.ds(0, rows)), (0, pl.ds(0, rows // 2)), (0, pl.ds(rows // 2, rows // 2)))

    def ring_send(step, p):
        dz, at = parts[p]
        ring[step, p] = arrival()
        for d in range(2):
            block = terms.at[level_of(NX - step if d == 0 else step, dz), at, col(d)]
            send(block, partial.at[d, step - 1, 1 - dz, at], x_up if d == 0 else x_down, ring[step, p])

    ring = {}
    spans = (pl.ds(0, 1), pl.ds(1, 1), pl.ds(2, 1), pl.ds(3, 1), pl.ds(4, 2), pl.ds(6, 1))
    low, high = pl.ds(0, shard // 2), pl.ds(shard // 2, shard // 2)

    quarter = width // NX
    all_rows, all_lanes = pl.ds(0, shard), pl.ds(0, width)

    def quarter_at(dx):
        return pl.ds(pl.multiple_of(lax.rem(xx + dx + NX, NX) * quarter, LANES), quarter)

    def lanes(g):
        return quarter_at(0) if g == JOIN else all_lanes

    def blocks(at, g, part=all_rows):
        return weights.at[at, core, spans[g], part, lanes(g)]

    def place(dz, dy, g, part=all_rows):
        at = lax.rem(zh + dz + NZ, NZ) * NY + lax.rem(yy + dy + NY, NY)
        return blocks(at, g, part)

    znear, zfar, ynear, yfar, mate = {}, {}, {}, {}, {}

    def z_start(g):
        block = place(0, 0, g)
        znear[g] = arrival()
        send(block, block, z_up, znear[g])
        send(block, block, z_down, znear[g])

    def z_forward(g):
        await_bytes(blocks(pl.ds(0, 2), g), znear[g])
        one, two = place(-1, 0, g, low), place(1, 0, g, high)
        zfar[g] = arrival()
        send(one, one, z_up, zfar[g])
        send(two, two, z_down, zfar[g])

    def z_last(g):
        await_bytes(blocks(0, g), zfar[g])

    def y_start(g, dz):
        block = place(dz, 0, g)
        ynear[g, dz] = arrival()
        send(block, block, y_up, ynear[g, dz])
        send(block, block, y_down, ynear[g, dz])

    def y_forward(g, dz):
        await_bytes(blocks(pl.ds(0, 2), g), ynear[g, dz])
        one, two = place(dz, -1, g, low), place(dz, 1, g, high)
        yfar[g, dz] = arrival()
        send(one, one, y_up, yfar[g, dz])
        send(two, two, y_down, yfar[g, dz])

    def mate_start(g, dz):
        await_bytes(blocks(0, g), yfar[g, dz])
        plane = weights.at[pl.ds(lax.rem(zh + dz + NZ, NZ) * NY, NY), core, spans[g]]
        if g not in mate:
            mate[g] = arrival()
        send(plane, plane, core_mate, mate[g])

    x_sems = []

    def x_start():
        for dz in (0, -1, 1, 2):
            await_bytes(blocks(0, JOIN), yfar[JOIN, dz])
        x_sems.extend([arrival(), arrival()])
        block = weights.at[:, core, 6, :, quarter_at(0)]
        send(block, block, x_up, x_sems[0])
        send(block, block, x_down, x_sems[0])

    def x_forward():
        half_at = NZ * NY // 2
        await_bytes(weights.at[:, core, 6, :, pl.ds(0, 2 * quarter)], x_sems[0])
        one = weights.at[pl.ds(0, half_at), core, 6, :, quarter_at(-1)]
        two = weights.at[pl.ds(half_at, half_at), core, 6, :, quarter_at(1)]
        send(one, one, x_up, x_sems[1])
        send(two, two, x_down, x_sems[1])

    def x_mate():
        await_bytes(weights.at[:, core, 6, :, pl.ds(0, quarter)], x_sems[1])
        mate[JOIN] = arrival()
        block = weights.at[:, core, 6]
        send(block, block, core_mate, mate[JOIN])

    def mate_wait(g):
        await_bytes(weights.at[:, core, spans[g]], mate[g])

    z_sem = arrival()

    def ring_next(step, p):
        dz, at = parts[p]
        await_bytes(partial.at[:, step - 1, 1 - dz, at], ring[step, p])
        for d in range(2):
            dest = level_of(2 * NX - step - 1 if d == 0 else step + 1, dz)
            total = terms[dest, at, col(d)].astype(F32) + partial[d, step - 1, 1 - dz, at].astype(F32)
            if step < NX - 1:
                terms[dest, at, col(d)] = total.astype(BF16)
            elif dz == 1:
                zsend[d] = total.astype(BF16)
                send(zsend.at[d], zrecv.at[d], z_mate, z_sem)
            else:
                own[pl.ds(edge + at.start, at.size), col(d)] = total
        if step < NX - 1:
            ring_send(step + 1, p)

    pl.semaphore_wait(barrier, groups + 4)
    for load in loads[1:6]:
        load.wait()

    def columns_start(j, count):
        block = weights.at[zy, core, pl.ds(j, count), :, lane_at]
        sem = arrival()
        for k in range(1, groups):
            send(block, block, {"level": level_of(k // NL, k % NL)}, sem)
        return sem

    def columns_wait(j, count, sem):
        await_bytes(weights.at[zy, core, pl.ds(j, count), :, pl.ds(0, (groups - 1) * LANES)], sem)

    qkv_columns = columns_start(0, 3)
    y_start(EXPAND, 0)
    y_start(JOIN, 0)
    loads[0].wait()

    def first_terms(first, last):
        @pl.loop(first, last)
        def _(i):
            term(2 * lax.rem(i, 2) + NX - 1, 1 - i // 2)

    first_terms(0, 2)
    ring_send(1, 0)
    out_columns = columns_start(3, 1)
    first_terms(2, 4)
    ring_send(1, 1)
    columns_wait(0, 3, qkv_columns)
    for g in (K, Q):
        z_start(g)
        y_start(g, 0)
    z_start(JOIN)
    z_start(V)
    y_start(V, 0)

    @pl.loop(0, 4)
    def _(i):
        term(2 + 2 * (i // 2), lax.rem(i + 1, 2))

    ring_next(1, 0)
    ring_send(1, 2)
    y_forward(K, 0)
    y_forward(Q, 0)
    z_forward(K)
    y_start(K, -1)
    y_start(K, 1)
    y_forward(V, 0)
    y_forward(JOIN, 0)
    z_forward(Q)
    y_start(Q, -1)
    y_start(Q, 1)
    ring_next(2, 0)
    ring_next(1, 1)
    z_forward(JOIN)
    y_start(JOIN, -1)
    y_start(JOIN, 1)
    z_forward(V)
    y_start(V, -1)
    y_start(V, 1)
    ring_next(1, 2)
    columns_wait(3, 1, out_columns)
    z_start(OUT)
    mate_start(K, 0)
    mate_start(Q, 0)
    mate_start(V, 0)
    z_last(K)
    y_start(K, 2)
    z_last(Q)
    y_start(Q, 2)
    y_forward(K, -1)
    y_forward(K, 1)
    z_last(JOIN)
    y_start(JOIN, 2)
    z_last(V)
    y_start(V, 2)
    ring_next(3, 0)
    z_start(EXPAND)
    ring_next(2, 1)
    y_forward(Q, -1)
    y_forward(Q, 1)
    ring_next(2, 2)
    z_forward(OUT)
    y_forward(JOIN, -1)
    y_forward(JOIN, 1)
    y_forward(V, -1)
    y_forward(V, 1)
    y_forward(K, 2)
    y_forward(Q, 2)
    ring_next(3, 1)
    y_forward(JOIN, 2)
    y_forward(V, 2)
    for dz in (0, -1, 1):
        y_start(OUT, dz)
    y_forward(EXPAND, 0)
    mate_start(K, -1)
    mate_start(K, 1)
    mate_start(Q, -1)
    mate_start(Q, 1)
    ring_next(3, 2)
    mate_start(K, 2)
    mate_start(Q, 2)
    x_start()
    mate_start(V, -1)
    mate_start(V, 1)
    mate_start(V, 2)
    await_bytes(zrecv, z_sem)
    for d in range(2):
        own[inner, col(d)] += zrecv[d].astype(F32)

    chunk = rows // 2

    @pl.loop(0, rows // chunk)
    def _(i):
        at = pl.ds(pl.multiple_of(edge + i * chunk, 16), chunk)
        normed[at] = layer_norm(own[at]).astype(BF16)

    mate_wait(K)

    def weight(j, start, size):
        return weights[:, :, j, :, pl.ds(start, size)].reshape(width, size)

    def project(j):
        size = half
        for h in range(width // size):
            product = jnp.dot(normed[inner], weight(j, h * size, size), preferred_element_type=F32)
            for i in range(size // LANES):
                qkv_s[h * (size // LANES) + i, j] = product[:, i * LANES : (i + 1) * LANES].astype(BF16)

    def exchange(j, sems):
        for i in range(1, groups):
            k = 3 * i % groups
            dest = level_of(k // NL, k % NL)
            send(qkv_s.at[dest, j], qkv_r.at[lv, j], {"level": dest}, sems[k % len(sems)])
        qkv_r[lv, j] = qkv_s[lv, j]

    def level_of_index(at):
        return lax.rem(at + groups, groups)

    k_sem = arrival()
    project(1)
    exchange(1, (k_sem,))
    z_forward(EXPAND)
    y_start(EXPAND, -1)
    y_start(EXPAND, 1)
    mate_wait(Q)
    project(0)
    q_base = len(arrivals)
    exchange(0, [arrival() for _ in range(groups)])
    mate_wait(V)
    project(2)
    v_sem = arrival()
    exchange(2, (v_sem,))
    side = (level_of_index(lv + 1), level_of_index(lv - 1))
    edge_sem = arrival()
    send(own.at[pl.ds(rows, edge)], own.at[pl.ds(0, edge)], {"level": side[0]}, edge_sem)
    send(own.at[pl.ds(edge, edge)], own.at[pl.ds(edge + rows, edge)], {"level": side[1]}, edge_sem)
    z_last(OUT)
    y_start(OUT, 2)
    for dz in (0, -1, 1):
        y_forward(OUT, dz)
    await_bytes(qkv_r.at[pl.ds(0, groups - 1), 1], k_sem)

    head_dim = width // HEADS
    att_sem, att_low, att_high = arrival(), arrival(), arrival()
    heads = LANES // head_dim

    def source(k):
        return level_of(NX - k // NL, NL - lax.rem(k, NL))

    def lane_head():
        return lax.broadcasted_iota(jnp.int32, (rows, LANES), 1) // head_dim

    def score(k):
        src = source(k)
        query = qkv_r[src, 0].astype(F32) * head_dim ** (-0.5)
        keys = qkv_r[:, 1].reshape(frames, LANES)
        total = jnp.zeros((rows, LANES), F32)
        for h in range(heads):
            masked = jnp.where(lane_head() == h, query, 0.0).astype(BF16)
            scores = lax.dot_general(masked, keys, (((1,), (1,)), ((), ())), preferred_element_type=F32)
            grown = jnp.exp(scores - jnp.max(scores, axis=-1, keepdims=True))
            probs[src, h] = grown.astype(BF16)
            total = jnp.where(lane_head() == h, jnp.sum(grown, axis=-1, keepdims=True), total)
        sums[src] = total

    def mix(k):
        src = source(k)
        values = qkv_r[:, 2].reshape(frames, LANES)
        merged = jnp.dot(probs[src, 0], values, preferred_element_type=F32)
        for h in range(1, heads):
            merged = jnp.where(lane_head() == h, jnp.dot(probs[src, h], values, preferred_element_type=F32), merged)
        return (merged / sums[src]).astype(BF16)

    def send_edges(src, out_low, out_high):
        block = att_s.at[src]
        for rows_at, lands, to, out_sem, in_sem in (
            (pl.ds(rows - edge, edge), pl.ds(0, edge), level_of_index(src + 1), out_low, att_low),
            (pl.ds(0, edge), pl.ds(edge + rows, edge), level_of_index(src - 1), out_high, att_high),
        ):

            @pl.when(to != lv)
            def _():
                make(block.at[rows_at], att_r.at[lands, lane_at], {"level": to}, out_sem, in_sem).start()

            @pl.when(to == lv)
            def _():
                att_r[lands, lane_at] = att_s[src, rows_at]

    def mix_send(k):
        src = source(k)
        att_s[src] = mix(k)
        make(att_s.at[src], att_r.at[inner, lane_at], {"level": src}, att_send.at[0], att_sem).start()
        send_edges(src, att_send.at[1], att_send.at[2])

    def scores_of(first, last):
        @pl.loop(first, last)
        def _(i):
            k = lax.rem(3 * i, groups)
            src = source(k)
            make(qkv_s.at[src, 0], qkv_r.at[src, 0], {"level": src}, send_sem.at[0], recv_sem.at[q_base + k]).wait_recv()
            score(k)

    def mixes_of(first, last):
        @pl.loop(first, last)
        def _(i):
            mix_send(lax.rem(3 * i, groups))

    score(0)
    scores_of(1, 3)
    x_forward()
    mate_start(EXPAND, 0)
    y_forward(OUT, 2)
    mate_start(OUT, 0)
    y_forward(EXPAND, -1)
    y_forward(EXPAND, 1)
    scores_of(3, 5)
    mate_start(OUT, -1)
    mate_start(OUT, 1)
    z_last(EXPAND)
    y_start(EXPAND, 2)
    scores_of(5, groups)
    await_bytes(qkv_r.at[pl.ds(0, groups - 1), 2], v_sem)
    mixes_of(1, 4)
    mate_start(OUT, 2)
    y_forward(EXPAND, 2)
    mate_start(EXPAND, -1)
    mate_start(EXPAND, 1)
    x_mate()
    mixes_of(4, groups)
    att_s[lv] = mix(0)
    send_edges(lv, att_send.at[1], att_send.at[2])
    att_r[inner, lane_at] = att_s[lv]
    mate_start(EXPAND, 2)
    others = pl.ds(0, (groups - 1) * LANES)
    await_bytes(att_r.at[inner, others], att_sem)
    await_bytes(att_r.at[pl.ds(0, edge), others], att_low)
    await_bytes(att_r.at[pl.ds(0, edge), others], att_high)
    await_bytes(own.at[pl.ds(0, 2 * edge)], edge_sem)
    mate_wait(OUT)

    attended = lax.dot_general(
        att_r[...], weight(3, 0, width), (((1,), (1,)), ((), ())), preferred_element_type=F32
    )
    after[...] = own[...] + attended

    part = wide // 2

    @pl.loop(0, wide // part)
    def _(i):
        at = pl.ds(pl.multiple_of(i * part, 16), part)
        normed[at] = layer_norm(after[at]).astype(BF16)

    mate_wait(EXPAND)
    piece = 256
    for h in range(width // piece):
        at = pl.ds(h * piece, piece)
        linear = jnp.dot(normed[...], weight(4, h * piece, piece), preferred_element_type=F32)
        gate = jnp.dot(normed[...], weight(5, h * piece, piece), preferred_element_type=F32)
        padded[:, at] = (linear * jax.nn.sigmoid(gate)).astype(BF16).astype(F32)
    padded[pl.ds(0, edge)] = jnp.where(lv > 0, padded[pl.ds(0, edge)], 0.0)
    padded[pl.ds(edge + rows, edge)] = jnp.where(lv < groups - 1, padded[pl.ds(edge + rows, edge)], 0.0)

    taps = taps_ref.shape[0]
    reach = taps // 2

    def convolve(start, count):
        conv = jnp.zeros((count, width), F32)
        for t in range(taps):
            conv = conv + padded[pl.ds(edge + start + t - reach, count)] * taps_ref[pl.ds(t, 1)].astype(F32)
        active[pl.ds(start, count)] = (conv * jax.nn.sigmoid(conv)).astype(BF16)

    mate_wait(JOIN)

    part = rows // 2
    share = part // 6 // EDGE * EDGE
    side_sems, mate_sems, far_sems, last_sems, tail_sems, cross_sems = ([arrival(), arrival()] for _ in range(6))

    for n in range(2):
        at, wide_at = pl.ds(n * part, part), pl.ds(edge + n * part, part)
        for start in range(n * part, (n + 1) * part, 32):
            convolve(start, 32)
        after[wide_at] += jnp.dot(active[at], weight(6, 0, width), preferred_element_type=F32)
        final[lv, at] = layer_norm(after[wide_at]).astype(BF16)
        mine = final.at[lv, at]
        send(mine, mine, x_up, side_sems[n])
        send(mine, mine, x_down, side_sems[n])
        send(mine, mine, z_mate, mate_sems[n])

    def logits(block, start=0, count=rows):
        at = pl.ds(pl.multiple_of(block * rows + start, 32), count)
        states = final[block, pl.ds(start, count)]
        for h in range(2):
            product = jnp.dot(states, head[:, col(h)], preferred_element_type=F32)
            out[at, col(h)] = product.astype(BF16)

    loads[6].wait()
    logits(lv)
    for n in range(2):
        start, middle = n * part, n * part + part // 2
        await_bytes(final.at[pl.ds(0, 2), pl.ds(0, part)], side_sems[n])
        one = final.at[level_of(-1, 0), pl.ds(start, part // 2)]
        two = final.at[level_of(1, 0), pl.ds(middle, part // 2)]
        send(one, one, x_up, far_sems[n])
        send(two, two, x_down, far_sems[n])
        for dx in (-1, 1):
            tail = final.at[level_of(dx, 0), pl.ds(start + part - share, share)]
            send(tail, tail, z_mate, tail_sems[n])
    for n in range(2):
        await_bytes(final.at[0, pl.ds(0, part)], mate_sems[n])
        block = final.at[level_of(0, 1), pl.ds(n * part, part - share)]
        send(block, block, x_up, cross_sems[n])
        send(block, block, x_down, cross_sems[n])
    logits(level_of(-1, 0))
    logits(level_of(1, 0))
    for n in range(2):
        await_bytes(final.at[0, pl.ds(0, part)], far_sems[n])
        block = final.at[level_of(2, 0), pl.ds(n * part, part)]
        send(block, block, z_mate, last_sems[n])
        logits(level_of(2 * n, 1 - n))
    for n in range(2):
        await_bytes(final.at[pl.ds(0, 2), pl.ds(0, part - share)], cross_sems[n])
        await_bytes(final.at[pl.ds(0, 2), pl.ds(0, share)], tail_sems[n])
        logits(level_of(-1, 1), n * part, part)
        logits(level_of(1, 1), n * part, part)
        await_bytes(final.at[0, pl.ds(0, part)], last_sems[n])
        logits(level_of(2, 1), n * part, part)

    for copy in sent[-SENDS:]:
        copy.wait_send()
    for i, ref in enumerate((att_s.at[pl.ds(0, groups - 1)],) + (att_s.at[pl.ds(0, groups - 1), pl.ds(0, edge)],) * 2):
        make(ref, ref, core_mate, att_send.at[i], recv_sem.at[0]).wait_send()


def body(
    token_ids,
    decoded_mask,
    levels_done,
    code_tables,
    mask_vectors,
    w_qkv,
    w_out,
    w_expand,
    w_depth,
    w_project,
    level_heads,
):
    frames = token_ids.shape[2]
    width = code_tables.shape[2]
    groups = lax.axis_size("level")
    rows = frames // groups
    shard = w_project.shape[0]
    wide = rows + 2 * EDGE
    vmem = pl.BlockSpec(memory_space=pltpu.VMEM)
    hbm = pl.BlockSpec(memory_space=pl.ANY)
    logits = pl.pallas_call(
        step_kernel,
        out_shape=pltpu.VMEM((frames, level_heads.shape[2]), BF16),
        in_specs=[vmem] * 2 + [pl.BlockSpec(memory_space=pltpu.SMEM)] + [vmem] * 2 + [hbm] * 6,
        out_specs=vmem,
        scratch_shapes=[
            pltpu.VMEM(code_tables.shape[1:], BF16),
            pltpu.VMEM(level_heads.shape[1:], BF16),
            pltpu.VMEM((frames, LANES), F32),
            pltpu.VMEM((NZ * NY, NC, 7, shard, width), BF16),
            pltpu.VMEM((groups, rows, width), BF16),
            pltpu.VMEM((2, NX - 1, 2, rows, width // 2), BF16),
            pltpu.VMEM((2, rows, width // 2), BF16),
            pltpu.VMEM((2, rows, width // 2), BF16),
            pltpu.VMEM((wide, width), F32),
            pltpu.VMEM((wide, width), BF16),
            pltpu.VMEM((groups, 3, rows, LANES), BF16),
            pltpu.VMEM((groups, 3, rows, LANES), BF16),
            pltpu.VMEM((groups, rows, LANES), BF16),
            pltpu.VMEM((wide, width), BF16),
            pltpu.VMEM((wide, width), F32),
            pltpu.VMEM((wide, width), F32),
            pltpu.VMEM((rows, width), BF16),
            pltpu.VMEM((groups, rows, width), BF16),
            pltpu.VMEM((groups, LANES * HEADS // width, rows, frames), BF16),
            pltpu.VMEM((groups, rows, LANES), F32),
            pltpu.SemaphoreType.DMA((7,)),
            pltpu.SemaphoreType.DMA((SENDS,)),
            pltpu.SemaphoreType.DMA((ARRIVALS,)),
            pltpu.SemaphoreType.DMA((3,)),
        ],
        compiler_params=pltpu.CompilerParams(
            collective_id=0, has_side_effects=True, vmem_limit_bytes=60 * 1024 * 1024
        ),
    )(
        token_ids[0],
        decoded_mask[0],
        levels_done,
        mask_vectors,
        w_depth,
        code_tables[0],
        w_qkv,
        w_out.T,
        w_expand,
        w_project,
        level_heads[0],
    )
    return logits[None, None]


def solution(mesh):
    return jax.shard_map(
        body,
        mesh=mesh,
        in_specs=(
            P("dp", "level", None),
            P("dp", "level", None),
            P("dp"),
            P("level", None, None),
            P("level", None),
            P(None, "dp", "level"),
            P("level", "dp"),
            P("dp", None),
            P(),
            P("dp", None),
            P("level", None, None),
        ),
        out_specs=P("dp", "level", None, None),
        check_vma=False,
    )
```
